32 devices in a mesh: groups: 2 (over y), fibre: 4 (over z), seg: 2 (over x), rec: 2 (over core).
Axes of the slice: x: 2, y: 2, z: 4, core: 2. Of those that a mesh axis runs over, the one named last changes fastest.
Arguments:
- records: bfloat16 [2, 2048, 1024], P('rec', 'fibre', ('groups', 'seg')), parts along dimension 2, may hold values from -6 to 6
- pairs: int32 [16, 2], replicated, may hold values from 0 to 15
- observed: float32 [32, 32, 256], P(('groups', 'fibre', 'seg')), parts along dimension 0, may hold values from -6 to 6
- lag_mask: int32 [32, 256], P(('groups', 'fibre', 'seg')), parts along dimension 0, may hold values 0 or 1
Outputs:
- adjoint_sources: bfloat16 [2, 2048, 1024], P('rec', 'fibre', ('groups', 'seg')), parts along dimension 2
The draws below stay inside these ranges and needn't reach their ends.
There are 2 independent parts, one for each index of `groups`. The reference program is written for one: setup_inputs(seed, part) draws one part's arguments, and reference() takes and returns one part's arrays. A program takes and returns all parts, laid end to end along the dimension named above; an argument that names none is the same for every part. Nothing has to cross between parts.
All inputs are finite; a program needn't handle non-finite values. No bound on the sum of `lag_mask` on one device may be relied on, other than what follows from the above.
Results may differ from the reference program's by a relative error of at most 0.015.
Values may be sent and summed in bfloat16 or wider, within the bound.
A program may use at most 64 MiB of HBM per device.

```python
import jax
import jax.numpy as jnp

S = 2048
F = 1024
LAGS = 256
BLOCK = 32
CHANNELS = 512
NBLOCKS = 16
NPAIRS = 16


def set_ends(entries, own_key, least, largest):
    extent = entries.shape
    place = [jax.random.randint(jax.random.fold_in(own_key, axis), (), 0, extent[axis]) for axis in range(len(extent))]
    entries = entries.at[tuple(place)].set(least)
    longest = extent.index(max(extent))
    place[longest] = (place[longest] + 1) % extent[longest]
    return entries.at[tuple(place)].set(largest)


def steps_of(rng, shape, shards, low, top_value):
    loudness = 1.0
    for dim, shards_of in shards:
        steps = jax.random.uniform(jax.random.fold_in(jax.random.fold_in(rng, 6), dim), (shards_of,), jnp.float32, low / len(shards), top_value / len(shards))
        loudness = loudness * jnp.repeat(jnp.exp(steps), shape[dim] // shards_of).reshape((-1,) + (1,) * (len(shape) - 1 - dim))
    return loudness


def centred(stream_key, shape, deviation, limit, shards=(), kind=jnp.bfloat16):
    values = jax.random.normal(stream_key, shape, jnp.float32) * deviation
    if len(shards) > 0:
        values = steps_of(stream_key, shape, shards, -0.22, 0.18) * values
    return jnp.clip(values, min=-limit, max=limit).astype(kind)


def setup_inputs(seed: int = 0, part: int = 0) -> dict:
    streams_of = jax.random.split(jax.random.key(seed), 5)
    part_splits = jax.random.split(jax.random.fold_in(streams_of[4], part), 5)
    return {
        "records": centred(part_splits[0], (2, S, CHANNELS), 1.0, 6.0, ((0, 2), (1, 4), (2, 2))),
        "pairs": set_ends(jax.random.randint(streams_of[1], (NPAIRS, 2), 0, NBLOCKS), jax.random.fold_in(streams_of[1], 1), 0, NBLOCKS - 1).astype(jnp.int32),
        "observed": centred(part_splits[2], (NPAIRS, BLOCK, LAGS), 1.0, 6.0, ((0, 8),), jnp.float32),
        "lag_mask": set_ends((jax.random.randint(part_splits[3], (NPAIRS, LAGS), 0, 4) < 3).astype(jnp.int32), jax.random.fold_in(part_splits[3], 1), 0, 1),
    }


def forward_table():
    freq_index = jnp.arange(F, dtype=jnp.int32)
    time_index = jnp.arange(S, dtype=jnp.int32)
    phase = freq_index[:, None] * time_index[None, :] % S
    angles = phase.astype(jnp.float32) * (2.0 * jnp.pi / S)
    scale = 1.0 / jnp.sqrt(jnp.float32(S))
    return jnp.stack([(jnp.cos(angles) * scale).astype(jnp.bfloat16), (-jnp.sin(angles) * scale).astype(jnp.bfloat16)], axis=1)

def lag_table():
    freq_index = jnp.arange(F, dtype=jnp.int32)
    shifts = (jnp.arange(LAGS, dtype=jnp.int32) - LAGS // 2) % S
    phase = freq_index[:, None] * shifts[None, :] % S
    angles = phase.astype(jnp.float32) * (2.0 * jnp.pi / S)
    scale = 1.0 / jnp.sqrt(jnp.float32(F))
    return jnp.stack([(jnp.cos(angles) * scale).astype(jnp.bfloat16), (-jnp.sin(angles) * scale).astype(jnp.bfloat16)], axis=1)

def reference(records, pairs, observed, lag_mask):
    table = forward_table().astype(jnp.float32)
    lags = lag_table().astype(jnp.float32)
    spectra = jnp.einsum('wps,rsc->rwpc', table, records.astype(jnp.float32)).astype(jnp.bfloat16)
    blocks_grid = spectra.reshape(2, F, 2, NBLOCKS, BLOCK)
    first_side = jnp.take(blocks_grid, pairs[:, 0], axis=3).astype(jnp.float32)
    second_side = jnp.take(blocks_grid, pairs[:, 1], axis=3).astype(jnp.float32)
    first_re, first_im = (first_side[:, :, 0], first_side[:, :, 1])
    second_re, second_im = (second_side[:, :, 0], second_side[:, :, 1])
    cross_re = first_re * second_re + first_im * second_im
    cross_im = first_im * second_re - first_re * second_im
    cross_spec = jnp.stack([cross_re, cross_im], axis=2).astype(jnp.bfloat16)
    synthetic = jnp.einsum('rwpnk,wpl->nkl', cross_spec.astype(jnp.float32), lags)
    weights = lag_mask[:, None, :].astype(jnp.float32) * jnp.tanh(synthetic - observed)
    weights_low = weights.astype(jnp.bfloat16)
    adjoint_cross = jnp.einsum('nkl,wpl->wpnk', weights_low.astype(jnp.float32), lags).astype(jnp.bfloat16)
    adjoint_re = adjoint_cross[:, 0].astype(jnp.float32)[None]
    adjoint_im = adjoint_cross[:, 1].astype(jnp.float32)[None]
    grad_first = jnp.stack([adjoint_re * second_re - adjoint_im * second_im, adjoint_re * second_im + adjoint_im * second_re], axis=2)
    grad_second = jnp.stack([adjoint_re * first_re + adjoint_im * first_im, adjoint_re * first_im - adjoint_im * first_re], axis=2)
    contributions = jnp.concatenate([grad_first, grad_second], axis=3)
    endpoint_ids = jnp.concatenate([pairs[:, 0], pairs[:, 1]]).astype(jnp.int32)
    summed = jax.ops.segment_sum(jnp.moveaxis(contributions, 3, 0), endpoint_ids, num_segments=NBLOCKS)
    block_adjoint = jnp.moveaxis(summed, 0, 3).astype(jnp.bfloat16).reshape(2, F, 2, CHANNELS)
    adjoint_sources = jnp.einsum('rwpc,wps->rsc', block_adjoint.astype(jnp.float32), table)
    return adjoint_sources.astype(jnp.bfloat16)
```

```python
import functools

import jax
import jax.numpy as jnp
import numpy as np
from jax import lax
from jax.experimental import pallas as pl
from jax.experimental.pallas import tpu as pltpu
from jax.sharding import PartitionSpec as P

S = 2048
F = 1024
LAGS = 256
BLOCK = 32
CH_DEV = 64


def forward_table():
    freq_index = jnp.arange(F, dtype=jnp.int32)
    time_index = jnp.arange(S, dtype=jnp.int32)
    phase = freq_index[:, None] * time_index[None, :] % S
    angles = phase.astype(jnp.float32) * (2.0 * jnp.pi / S)
    scale = 1.0 / jnp.sqrt(jnp.float32(S))
    return jnp.stack(
        [
            (jnp.cos(angles) * scale).astype(jnp.bfloat16),
            (-jnp.sin(angles) * scale).astype(jnp.bfloat16),
        ],
        axis=1,
    )


def lag_table():
    freq_index = jnp.arange(F, dtype=jnp.int32)
    shifts = (jnp.arange(LAGS, dtype=jnp.int32) - LAGS // 2) % S
    phase = freq_index[:, None] * shifts[None, :] % S
    angles = phase.astype(jnp.float32) * (2.0 * jnp.pi / S)
    scale = 1.0 / jnp.sqrt(jnp.float32(F))
    return jnp.stack(
        [
            (jnp.cos(angles) * scale).astype(jnp.bfloat16),
            (-jnp.sin(angles) * scale).astype(jnp.bfloat16),
        ],
        axis=1,
    )


def synthesize(incoming, table):
    count = incoming.shape[-1]
    flat = incoming.reshape(2 * F, count)
    result = jnp.einsum(
        "qn,qt->tn", flat, table.reshape(2 * F, S), preferred_element_type=jnp.float32
    )
    return result.astype(jnp.bfloat16)


def on_device(records, pairs, observed, lag_mask):
    fibre_count = lax.axis_size("fibre")
    seg_count = lax.axis_size("seg")
    spread_count = fibre_count * seg_count
    freq_dev = F // spread_count
    blocks_dev = CH_DEV // BLOCK
    block_count = CH_DEV * spread_count // BLOCK
    pair_total = pairs.shape[0]
    pairs_dev = pair_total // spread_count
    table = forward_table()
    lags = lag_table()
    spans = records.reshape(1, S // fibre_count, fibre_count, CH_DEV)
    incoming = lax.all_to_all(spans, "fibre", split_axis=2, concat_axis=1, tiled=True)
    count = incoming.shape[3]
    signal = incoming.reshape(S, count)
    result = jnp.einsum(
        "qs,sn->qn", table.reshape(2 * F, S), signal, preferred_element_type=jnp.float32
    )
    spectra = result.reshape(F, 2, count).astype(jnp.bfloat16)
    widened = lax.all_to_all(spectra, ("fibre", "seg"), split_axis=0, concat_axis=2, tiled=True)
    seg_blocks = fibre_count * blocks_dev
    slot_ids = (
        pairs % seg_blocks // blocks_dev * seg_count + pairs // seg_blocks
    ) * blocks_dev + pairs % blocks_dev
    blocks_grid = widened.reshape(freq_dev, 2, block_count, BLOCK)
    first_side = jnp.take(blocks_grid, slot_ids[:, 0], axis=2).astype(jnp.float32)
    second_side = jnp.take(blocks_grid, slot_ids[:, 1], axis=2).astype(jnp.float32)
    first_re, first_im = (first_side[:, 0], first_side[:, 1])
    second_re, second_im = (second_side[:, 0], second_side[:, 1])
    cross_re = first_re * second_re + first_im * second_im
    cross_im = first_im * second_re - first_re * second_im
    cross_spec = jnp.stack([cross_re, cross_im], axis=1).astype(jnp.bfloat16)
    cross_spec = cross_spec.reshape(freq_dev, 2, spread_count, pairs_dev * BLOCK)
    owned_spec = lax.all_to_all(
        cross_spec, ("fibre", "seg"), split_axis=2, concat_axis=0, tiled=True
    )
    owned_spec = owned_spec.reshape(F, 2, pairs_dev * BLOCK)
    partial_corr = jnp.einsum("wpx,wpl->xl", owned_spec, lags, preferred_element_type=jnp.float32)
    synthetic = (
        lax.psum(partial_corr.astype(jnp.bfloat16), "rec")
        .astype(jnp.float32)
        .reshape(pairs_dev, BLOCK, LAGS)
    )
    weights = lag_mask[:, None, :].astype(jnp.float32) * jnp.tanh(synthetic - observed)
    weights_low = weights.astype(jnp.bfloat16).reshape(pairs_dev * BLOCK, LAGS)
    adjoint_spec = jnp.einsum("xl,wpl->wpx", weights_low, lags, preferred_element_type=jnp.float32)
    adjoint_spec = adjoint_spec.astype(jnp.bfloat16).reshape(F, 2, 1, pairs_dev * BLOCK)
    returned = lax.all_to_all(
        adjoint_spec, ("fibre", "seg"), split_axis=0, concat_axis=2, tiled=True
    )
    returned = returned.reshape(freq_dev, 2, pair_total, BLOCK).astype(jnp.float32)
    adjoint_re, adjoint_im = (returned[:, 0], returned[:, 1])
    grad_first = jnp.stack(
        [
            adjoint_re * second_re - adjoint_im * second_im,
            adjoint_re * second_im + adjoint_im * second_re,
        ],
        axis=1,
    )
    grad_second = jnp.stack(
        [
            adjoint_re * first_re + adjoint_im * first_im,
            adjoint_re * first_im - adjoint_im * first_re,
        ],
        axis=1,
    )
    contributions = jnp.concatenate([grad_first, grad_second], axis=2)
    endpoint_ids = jnp.concatenate([slot_ids[:, 0], slot_ids[:, 1]])
    summed = jax.ops.segment_sum(
        jnp.moveaxis(contributions, 2, 0), endpoint_ids, num_segments=block_count
    )
    block_adjoint = jnp.moveaxis(summed, 0, 2).astype(jnp.bfloat16)
    outgoing = block_adjoint.reshape(freq_dev, 2, spread_count, CH_DEV)
    sources = synthesize(
        lax.all_to_all(outgoing, ("fibre", "seg"), split_axis=2, concat_axis=0, tiled=True), table
    )
    regrouped = lax.all_to_all(sources, "fibre", split_axis=0, concat_axis=1, tiled=True)
    return regrouped[None]


def angle_parts(freqs, times, scale):
    phase = (freqs[:, None].astype(np.int64) * times[None, :]) % S
    angles = phase.astype(np.float32) * np.float32(2.0 * np.pi / S)
    return np.stack([np.cos(angles) * scale, -np.sin(angles) * scale])


def band_tables(spread_count):
    order = np.concatenate([np.arange(0, F, 2), np.arange(1, F, 2)]).reshape(spread_count, -1)
    half = np.arange(S // 2)
    scale = np.float32(1.0) / np.sqrt(np.float32(S))
    forward = np.concatenate(
        [angle_parts(band, half, scale).reshape(-1, S // 2) for band in order]
    )
    backward = np.stack([forward[:F].T, forward[F:].T])
    shifts = (np.arange(LAGS) - LAGS // 2) % S
    lag_scale = np.float32(1.0) / np.sqrt(np.float32(F))
    lags = np.stack([angle_parts(band, shifts, lag_scale).reshape(-1, LAGS) for band in order])
    return [table.astype(jnp.bfloat16) for table in (forward, backward, lags)]


def dot(left, right, left_dim=1, right_dim=0):
    return lax.dot_general(
        left,
        right,
        (((left_dim,), (right_dim,)), ((), ())),
        preferred_element_type=jnp.float32,
    )


def fused_kernel(
    sizes, x, pairs, observed, mask, forward_hbm, backward_hbm, lags_hbm, out,
    forward, backward, lags, stage1, inbox1, signal, stage2, inbox2, picked, select, stage3, inbox3,
    inbox4, stage5, inbox5, stage6, inbox6, load_sem,
    send1, recv1, send2, recv2, send3, recv3, send4, recv4, send5, recv5, send6, recv6,
):
    fibres, segs, recs = sizes
    bands = fibres * segs
    owners = bands * recs
    g, f, s, r = (lax.axis_index(name) for name in ("groups", "fibre", "seg", "rec"))
    band = f * segs + s
    mine = band * recs + r
    span, width = x.shape
    rows = span // 2
    chans = width // fibres
    freqs = F // bands
    low = jnp.bfloat16

    def at(fibre, seg, rec):
        return (g, fibre, seg, rec)

    def at_band(index):
        return at(index // segs, index % segs, r)

    def push(src, dst, send, recv, device):
        copy = pltpu.make_async_remote_copy(
            src_ref=src, dst_ref=dst, send_sem=send, recv_sem=recv,
            device_id=device, device_id_type=pl.DeviceIdType.MESH,
        )
        copy.start()
        return copy

    def arrived(dst, recv):
        pltpu.make_async_remote_copy(
            src_ref=dst, dst_ref=dst, send_sem=recv, recv_sem=recv,
            device_id=at(f, s, 1 - r), device_id_type=pl.DeviceIdType.MESH,
        ).wait_recv()

    sends = []
    for j in range(fibres):
        part = x[:, j * chans : (j + 1) * chans]
        stage1[j] = jnp.concatenate([part[:rows], part[rows:]], axis=1)
    for d in range(1, fibres):
        j = (f + d) % fibres
        sends.append(push(stage1.at[j], inbox1.at[f], send1.at[d - 1], recv1.at[f], at(j, s, r)))
    loads = [
        pltpu.make_async_copy(forward_hbm, forward, load_sem.at[0]),
        pltpu.make_async_copy(lags_hbm.at[band], lags, load_sem.at[1]),
        pltpu.make_async_copy(backward_hbm, backward, load_sem.at[2]),
    ]
    for load in loads:
        load.start()
    inbox1[f] = stage1[f]

    total = select.shape[0]
    count = pairs.shape[0] * BLOCK
    lane = lax.broadcasted_iota(jnp.int32, (1, 2 * count), 1)
    target = lane
    for side in range(2):
        for n in range(pairs.shape[0]):
            first = side * count + n * BLOCK
            inside = (lane >= first) & (lane < first + BLOCK)
            target = jnp.where(inside, lane + (pairs[n, side] * BLOCK - first), target)
    row = lax.broadcasted_iota(jnp.int32, (total, 2 * count), 0)
    select[...] = jnp.where(row == target, 1.0, 0.0).astype(low)

    for d in range(1, fibres):
        k = (f + d) % fibres
        arrived(inbox1.at[k], recv1.at[k])
    for h in range(fibres // 2):
        early = inbox1[h].astype(jnp.float32)
        late = inbox1[h + fibres // 2].astype(jnp.float32)
        for parity, value in enumerate((early + late, early - late)):
            value = value.astype(low)
            base = parity * (S // 2) + h * span
            signal[base : base + rows] = value[:, :chans]
            signal[base + rows : base + span] = value[:, chans:]

    loads[0].wait()
    for d in list(range(1, bands)) + [0]:
        j = (band + d) % bands
        parity = j // (bands // 2)
        table = forward[pl.ds(pl.multiple_of(j * 2 * freqs, 2 * freqs), 2 * freqs), :]
        held = signal[pl.ds(pl.multiple_of(parity * (S // 2), S // 2), S // 2), :]
        result = dot(table, held).astype(low)
        packed = jnp.concatenate([result[:freqs], result[freqs:]], axis=1)
        if d == 0:
            inbox2[band] = packed
        else:
            stage2[d - 1] = packed
            sends.append(
                push(stage2.at[d - 1], inbox2.at[band], send2.at[d - 1], recv2.at[band], at_band(j))
            )
    for d in range(1, bands):
        k = (band + d) % bands
        arrived(inbox2.at[k], recv2.at[k])
    order = [fibre * segs + seg for seg in range(segs) for fibre in range(fibres)]
    spectra = jnp.concatenate(
        [
            jnp.concatenate([inbox2[k][:, p * chans : (p + 1) * chans] for k in order], axis=1)
            for p in range(2)
        ],
        axis=0,
    )
    picked[...] = dot(spectra, select[...])
    a0, a1 = (picked[:freqs, :count], picked[freqs:, :count])
    b0, b1 = (picked[:freqs, count:], picked[freqs:, count:])
    cross = jnp.concatenate([a0 * b0 + a1 * b1, a1 * b0 - a0 * b1], axis=0).astype(low)
    loads[1].wait()
    partial = dot(cross, lags[...], 0, 0).astype(low)
    stage3[...] = partial.reshape(stage3.shape)
    for d in range(1, owners):
        j = (mine + d) % owners
        device = at(j // (segs * recs), j // recs % segs, j % recs)
        sends.append(push(stage3.at[j], inbox3.at[mine], send3.at[d - 1], recv3.at[mine], device))
    inbox3[mine] = stage3[mine]
    for d in range(1, owners):
        k = (mine + d) % owners
        arrived(inbox3.at[k], recv3.at[k])
    synthetic = inbox3[0].astype(jnp.float32)
    for k in range(1, owners):
        synthetic += inbox3[k].astype(jnp.float32)
    window = mask[pl.ds(r, 1), :].astype(jnp.float32)
    inbox4[mine] = (window * jnp.tanh(synthetic - observed[r])).astype(low)
    for d in range(1, owners):
        j = (mine + d) % owners
        device = at(j // (segs * recs), j // recs % segs, j % recs)
        sends.append(push(inbox4.at[mine], inbox4.at[mine], send4.at[d - 1], recv4.at[mine], device))
    for d in range(1, owners):
        k = (mine + d) % owners
        arrived(inbox4.at[k], recv4.at[k])
    weights = inbox4[...].reshape(count, LAGS)
    adjoint = dot(lags[...], weights, 1, 1).astype(low).astype(jnp.float32)
    g0, g1 = (adjoint[:freqs], adjoint[freqs:])
    a0, a1 = (picked[:freqs, :count], picked[freqs:, :count])
    b0, b1 = (picked[:freqs, count:], picked[freqs:, count:])
    grads = jnp.concatenate(
        [
            jnp.concatenate([g0 * b0 - g1 * b1, g0 * a0 + g1 * a1], axis=1),
            jnp.concatenate([g0 * b1 + g1 * b0, g0 * a1 - g1 * a0], axis=1),
        ],
        axis=0,
    ).astype(low)
    summed = dot(grads, select[...], 1, 1).astype(low)
    for place, k in enumerate(order):
        cut = slice(place * chans, (place + 1) * chans)
        stage5[k] = jnp.concatenate([summed[:freqs, cut], summed[freqs:, cut]], axis=1)
    for d in range(1, bands):
        j = (band + d) % bands
        sends.append(push(stage5.at[j], inbox5.at[band], send5.at[d - 1], recv5.at[band], at_band(j)))
    inbox5[band] = stage5[band]
    loads[2].wait()
    for d in range(1, bands):
        k = (band + d) % bands
        arrived(inbox5.at[k], recv5.at[k])
    held = []
    for parity in range(2):
        pieces = []
        for k in range(parity * bands // 2, (parity + 1) * bands // 2):
            pieces += [inbox5[k][:, :chans], inbox5[k][:, chans:]]
        held.append(jnp.concatenate(pieces, axis=0))
    for h in range(fibres // 2):
        cut = slice(h * span, (h + 1) * span)
        even = dot(backward[0, cut], held[0])
        odd = dot(backward[1, cut], held[1])
        for late, value in enumerate((even + odd, even - odd)):
            value = value.astype(low)
            stage6[h + late * (fibres // 2)] = jnp.concatenate([value[:rows], value[rows:]], axis=1)
    for d in range(1, fibres):
        j = (f + d) % fibres
        sends.append(push(stage6.at[j], inbox6.at[f], send6.at[d - 1], recv6.at[f], at(j, s, r)))
    inbox6[f] = stage6[f]
    for d in range(1, fibres):
        k = (f + d) % fibres
        arrived(inbox6.at[k], recv6.at[k])
    out[:rows, :] = jnp.concatenate([inbox6[k][:, :chans] for k in range(fibres)], axis=1)
    out[rows:, :] = jnp.concatenate([inbox6[k][:, chans:] for k in range(fibres)], axis=1)
    for copy in sends:
        copy.wait_send()


def fused_on_device(mesh_shape, tables, records, pairs, observed, lag_mask):
    fibres, segs, recs = (mesh_shape[name] for name in ("fibre", "seg", "rec"))
    bands = fibres * segs
    owners = bands * recs
    _, span, width = records.shape
    freqs = F // bands
    chans = width // fibres
    count = pairs.shape[0] * BLOCK
    low = jnp.bfloat16
    vmem = pl.BlockSpec(memory_space=pltpu.VMEM)
    hbm = pl.BlockSpec(memory_space=pltpu.HBM)
    row = (freqs, 2 * chans)
    slab = (span // 2, 2 * chans)
    corr = (BLOCK, LAGS)

    def sems(size):
        return [pltpu.SemaphoreType.DMA((size - 1,)), pltpu.SemaphoreType.DMA((size,))]

    result = pl.pallas_call(
        functools.partial(fused_kernel, (fibres, segs, recs)),
        out_shape=jax.ShapeDtypeStruct((span, width), low),
        in_specs=[vmem, pl.BlockSpec(memory_space=pltpu.SMEM), vmem, vmem, hbm, hbm, hbm],
        out_specs=vmem,
        scratch_shapes=[
            pltpu.VMEM((2 * F, S // 2), low),
            pltpu.VMEM((2, S // 2, F), low),
            pltpu.VMEM((2 * freqs, LAGS), low),
            pltpu.VMEM((fibres,) + slab, low),
            pltpu.VMEM((fibres,) + slab, low),
            pltpu.VMEM((S, chans), low),
            pltpu.VMEM((bands - 1,) + row, low),
            pltpu.VMEM((bands,) + row, low),
            pltpu.VMEM((2 * freqs, 2 * count), jnp.float32),
            pltpu.VMEM((segs * width, 2 * count), low),
            pltpu.VMEM((owners,) + corr, low),
            pltpu.VMEM((owners,) + corr, low),
            pltpu.VMEM((owners,) + corr, low),
            pltpu.VMEM((bands,) + row, low),
            pltpu.VMEM((bands,) + row, low),
            pltpu.VMEM((fibres,) + slab, low),
            pltpu.VMEM((fibres,) + slab, low),
            pltpu.SemaphoreType.DMA((3,)),
            *sems(fibres), *sems(bands), *sems(owners), *sems(owners), *sems(bands), *sems(fibres),
        ],
        compiler_params=pltpu.CompilerParams(
            has_side_effects=True, vmem_limit_bytes=40 * 1024 * 1024
        ),
        name="adjoint",
    )(records[0], pairs, observed, lag_mask, *tables)
    return result[None]


def fits_fused(shape, records, pairs):
    fibres, segs, recs = (shape[name] for name in ("fibre", "seg", "rec"))
    chans = records.shape[2] // (shape["groups"] * segs * fibres)
    return (
        fibres == 4
        and recs == 2
        and 2 * chans == 128
        and pairs.shape[0] == fibres * segs * recs
        and F // (fibres * segs) >= 16
    )


def solution(mesh):
    in_specs = (
        P("rec", "fibre", ("groups", "seg")),
        P(),
        P(("groups", "fibre", "seg"), None, None),
        P(("groups", "fibre", "seg"), None),
    )
    out_specs = P("rec", "fibre", ("groups", "seg"))
    shape = dict(mesh.shape)

    def run(records, pairs, observed, lag_mask):
        args = (records, pairs, observed, lag_mask)
        if not fits_fused(shape, records, pairs):
            return jax.shard_map(
                on_device, mesh=mesh, in_specs=in_specs, out_specs=out_specs, check_vma=False
            )(*args)
        tables = [jnp.asarray(t) for t in band_tables(shape["fibre"] * shape["seg"])]

        def body(*blocks):
            return fused_on_device(shape, tables, *blocks)

        return jax.shard_map(
            body, mesh=mesh, in_specs=in_specs, out_specs=out_specs, check_vma=False
        )(*args)

    return run
```

```python
import functools

import jax
import jax.numpy as jnp
import numpy as np
from jax import lax
from jax.experimental import pallas as pl
from jax.experimental.pallas import tpu as pltpu
from jax.sharding import PartitionSpec as P

S = 2048
F = 1024
LAGS = 256
BLOCK = 32
CH_DEV = 64
VMEM_GRANT = 67_043_328


def forward_table():
    freq_index = jnp.arange(F, dtype=jnp.int32)
    time_index = jnp.arange(S, dtype=jnp.int32)
    phase = freq_index[:, None] * time_index[None, :] % S
    angles = phase.astype(jnp.float32) * (2.0 * jnp.pi / S)
    scale = 1.0 / jnp.sqrt(jnp.float32(S))
    return jnp.stack(
        [
            (jnp.cos(angles) * scale).astype(jnp.bfloat16),
            (-jnp.sin(angles) * scale).astype(jnp.bfloat16),
        ],
        axis=1,
    )


def lag_table():
    freq_index = jnp.arange(F, dtype=jnp.int32)
    shifts = (jnp.arange(LAGS, dtype=jnp.int32) - LAGS // 2) % S
    phase = freq_index[:, None] * shifts[None, :] % S
    angles = phase.astype(jnp.float32) * (2.0 * jnp.pi / S)
    scale = 1.0 / jnp.sqrt(jnp.float32(F))
    return jnp.stack(
        [
            (jnp.cos(angles) * scale).astype(jnp.bfloat16),
            (-jnp.sin(angles) * scale).astype(jnp.bfloat16),
        ],
        axis=1,
    )


def synthesize(incoming, table):
    count = incoming.shape[-1]
    flat = incoming.reshape(2 * F, count)
    result = jnp.einsum(
        "qn,qt->tn", flat, table.reshape(2 * F, S), preferred_element_type=jnp.float32
    )
    return result.astype(jnp.bfloat16)


def on_device(records, pairs, observed, lag_mask):
    fibre_count = lax.axis_size("fibre")
    seg_count = lax.axis_size("seg")
    spread_count = fibre_count * seg_count
    freq_dev = F // spread_count
    blocks_dev = CH_DEV // BLOCK
    block_count = CH_DEV * spread_count // BLOCK
    pair_total = pairs.shape[0]
    pairs_dev = pair_total // spread_count
    table = forward_table()
    lags = lag_table()
    spans = records.reshape(1, S // fibre_count, fibre_count, CH_DEV)
    incoming = lax.all_to_all(spans, "fibre", split_axis=2, concat_axis=1, tiled=True)
    count = incoming.shape[3]
    signal = incoming.reshape(S, count)
    result = jnp.einsum(
        "qs,sn->qn", table.reshape(2 * F, S), signal, preferred_element_type=jnp.float32
    )
    spectra = result.reshape(F, 2, count).astype(jnp.bfloat16)
    widened = lax.all_to_all(spectra, ("fibre", "seg"), split_axis=0, concat_axis=2, tiled=True)
    seg_blocks = fibre_count * blocks_dev
    slot_ids = (
        pairs % seg_blocks // blocks_dev * seg_count + pairs // seg_blocks
    ) * blocks_dev + pairs % blocks_dev
    blocks_grid = widened.reshape(freq_dev, 2, block_count, BLOCK)
    first_side = jnp.take(blocks_grid, slot_ids[:, 0], axis=2).astype(jnp.float32)
    second_side = jnp.take(blocks_grid, slot_ids[:, 1], axis=2).astype(jnp.float32)
    first_re, first_im = (first_side[:, 0], first_side[:, 1])
    second_re, second_im = (second_side[:, 0], second_side[:, 1])
    cross_re = first_re * second_re + first_im * second_im
    cross_im = first_im * second_re - first_re * second_im
    cross_spec = jnp.stack([cross_re, cross_im], axis=1).astype(jnp.bfloat16)
    cross_spec = cross_spec.reshape(freq_dev, 2, spread_count, pairs_dev * BLOCK)
    owned_spec = lax.all_to_all(
        cross_spec, ("fibre", "seg"), split_axis=2, concat_axis=0, tiled=True
    )
    owned_spec = owned_spec.reshape(F, 2, pairs_dev * BLOCK)
    partial_corr = jnp.einsum("wpx,wpl->xl", owned_spec, lags, preferred_element_type=jnp.float32)
    synthetic = (
        lax.psum(partial_corr.astype(jnp.bfloat16), "rec")
        .astype(jnp.float32)
        .reshape(pairs_dev, BLOCK, LAGS)
    )
    weights = lag_mask[:, None, :].astype(jnp.float32) * jnp.tanh(synthetic - observed)
    weights_low = weights.astype(jnp.bfloat16).reshape(pairs_dev * BLOCK, LAGS)
    adjoint_spec = jnp.einsum("xl,wpl->wpx", weights_low, lags, preferred_element_type=jnp.float32)
    adjoint_spec = adjoint_spec.astype(jnp.bfloat16).reshape(F, 2, 1, pairs_dev * BLOCK)
    returned = lax.all_to_all(
        adjoint_spec, ("fibre", "seg"), split_axis=0, concat_axis=2, tiled=True
    )
    returned = returned.reshape(freq_dev, 2, pair_total, BLOCK).astype(jnp.float32)
    adjoint_re, adjoint_im = (returned[:, 0], returned[:, 1])
    grad_first = jnp.stack(
        [
            adjoint_re * second_re - adjoint_im * second_im,
            adjoint_re * second_im + adjoint_im * second_re,
        ],
        axis=1,
    )
    grad_second = jnp.stack(
        [
            adjoint_re * first_re + adjoint_im * first_im,
            adjoint_re * first_im - adjoint_im * first_re,
        ],
        axis=1,
    )
    contributions = jnp.concatenate([grad_first, grad_second], axis=2)
    endpoint_ids = jnp.concatenate([slot_ids[:, 0], slot_ids[:, 1]])
    summed = jax.ops.segment_sum(
        jnp.moveaxis(contributions, 2, 0), endpoint_ids, num_segments=block_count
    )
    block_adjoint = jnp.moveaxis(summed, 0, 2).astype(jnp.bfloat16)
    outgoing = block_adjoint.reshape(freq_dev, 2, spread_count, CH_DEV)
    sources = synthesize(
        lax.all_to_all(outgoing, ("fibre", "seg"), split_axis=2, concat_axis=0, tiled=True), table
    )
    regrouped = lax.all_to_all(sources, "fibre", split_axis=0, concat_axis=1, tiled=True)
    return regrouped[None]


def angle_parts(freqs, times, scale):
    phase = (freqs[:, None].astype(np.int64) * times[None, :]) % S
    angles = phase.astype(np.float32) * np.float32(2.0 * np.pi / S)
    return np.stack([np.cos(angles) * scale, -np.sin(angles) * scale])


def band_tables(spread_count):
    order = np.concatenate([np.arange(0, F, 2), np.arange(1, F, 2)]).reshape(spread_count, -1)
    half = np.arange(S // 2)
    scale = np.float32(1.0) / np.sqrt(np.float32(S))
    forward = np.concatenate(
        [angle_parts(band, half, scale).reshape(-1, S // 2) for band in order]
    )
    backward = np.stack([forward[:F].T, forward[F:].T])
    shifts = (np.arange(LAGS) - LAGS // 2) % S
    lag_scale = np.float32(1.0) / np.sqrt(np.float32(F))
    lags = np.stack([angle_parts(band, shifts, lag_scale).reshape(-1, LAGS) for band in order])
    return [table.astype(jnp.bfloat16) for table in (forward, backward, lags)]


def dot(left, right, left_dim=1, right_dim=0):
    return lax.dot_general(
        left,
        right,
        (((left_dim,), (right_dim,)), ((), ())),
        preferred_element_type=jnp.float32,
    )


def fused_kernel(
    sizes, x_hbm, pairs, observed_hbm, mask_hbm, forward_hbm, backward_hbm, lags_hbm, out,
    x, observed, mask, forward, backward, lags, stage1, inbox1, signal, stage2, inbox2, picked, select, stage3, inbox3,
    inbox4, stage5, inbox5, stage6, inbox6, load_sem,
    send1, recv1, send2, recv2, send3, recv3, send4, recv4, send5, recv5, send6, recv6,
):
    fibres, segs, recs = sizes
    bands = fibres * segs
    owners = bands * recs
    g, f, s, r = (lax.axis_index(name) for name in ("groups", "fibre", "seg", "rec"))
    band = f * segs + s
    mine = band * recs + r
    span, width = x.shape
    rows = span // 2
    chans = width // fibres
    freqs = F // bands
    low = jnp.bfloat16

    def at(fibre, seg, rec):
        return (g, fibre, seg, rec)

    def at_band(index):
        return at(index // segs, index % segs, r)

    def push(src, dst, send, recv, device):
        copy = pltpu.make_async_remote_copy(
            src_ref=src, dst_ref=dst, send_sem=send, recv_sem=recv,
            device_id=device, device_id_type=pl.DeviceIdType.MESH,
        )
        copy.start()
        return copy

    def arrived(dst, recv):
        pltpu.make_async_remote_copy(
            src_ref=dst, dst_ref=dst, send_sem=recv, recv_sem=recv,
            device_id=at(f, s, 1 - r), device_id_type=pl.DeviceIdType.MESH,
        ).wait_recv()

    sends = []
    first_load = pltpu.make_async_copy(x_hbm, x, load_sem.at[0])
    first_load.start()
    loads = [
        pltpu.make_async_copy(forward_hbm, forward, load_sem.at[1]),
        pltpu.make_async_copy(lags_hbm.at[band], lags, load_sem.at[2]),
        pltpu.make_async_copy(observed_hbm.at[r], observed, load_sem.at[3]),
        pltpu.make_async_copy(mask_hbm, mask, load_sem.at[4]),
        pltpu.make_async_copy(backward_hbm, backward, load_sem.at[5]),
    ]
    first_load.wait()
    for load in loads:
        load.start()
    for j in range(fibres):
        part = x[:, j * chans : (j + 1) * chans]
        stage1[j] = jnp.concatenate([part[:rows], part[rows:]], axis=1)
    for d in range(1, fibres):
        j = (f + d) % fibres
        sends.append(push(stage1.at[j], inbox1.at[f], send1.at[d - 1], recv1.at[f], at(j, s, r)))
    inbox1[f] = stage1[f]

    total = select.shape[0]
    count = pairs.shape[1] * BLOCK
    lane = lax.broadcasted_iota(jnp.int32, (1, 2 * count), 1)
    target = lane
    for side in range(2):
        for n in range(pairs.shape[1]):
            first = side * count + n * BLOCK
            inside = (lane >= first) & (lane < first + BLOCK)
            target = jnp.where(inside, lane + (pairs[side, n] * BLOCK - first), target)
    row = lax.broadcasted_iota(jnp.int32, (total, 2 * count), 0)
    select[...] = jnp.where(row == target, 1.0, 0.0).astype(low)

    for d in range(1, fibres):
        k = (f + d) % fibres
        arrived(inbox1.at[k], recv1.at[k])
    for h in range(fibres // 2):
        early = inbox1[h].astype(jnp.float32)
        late = inbox1[h + fibres // 2].astype(jnp.float32)
        for parity, value in enumerate((early + late, early - late)):
            value = value.astype(low)
            base = parity * (S // 2) + h * span
            signal[base : base + rows] = value[:, :chans]
            signal[base + rows : base + span] = value[:, chans:]

    loads[0].wait()
    for d in list(range(1, bands)) + [0]:
        j = (band + d) % bands
        parity = j // (bands // 2)
        table = forward[pl.ds(pl.multiple_of(j * 2 * freqs, 2 * freqs), 2 * freqs), :]
        held = signal[pl.ds(pl.multiple_of(parity * (S // 2), S // 2), S // 2), :]
        result = dot(table, held).astype(low)
        packed = jnp.concatenate([result[:freqs], result[freqs:]], axis=1)
        if d == 0:
            inbox2[band] = packed
        else:
            stage2[d - 1] = packed
            sends.append(
                push(stage2.at[d - 1], inbox2.at[band], send2.at[d - 1], recv2.at[band], at_band(j))
            )
    for d in range(1, bands):
        k = (band + d) % bands
        arrived(inbox2.at[k], recv2.at[k])
    order = [fibre * segs + seg for seg in range(segs) for fibre in range(fibres)]
    spectra = jnp.concatenate(
        [
            jnp.concatenate([inbox2[k][:, p * chans : (p + 1) * chans] for k in order], axis=1)
            for p in range(2)
        ],
        axis=0,
    )
    picked[...] = dot(spectra, select[...])
    a0, a1 = (picked[:freqs, :count], picked[freqs:, :count])
    b0, b1 = (picked[:freqs, count:], picked[freqs:, count:])
    cross = jnp.concatenate([a0 * b0 + a1 * b1, a1 * b0 - a0 * b1], axis=0).astype(low)
    loads[1].wait()
    partial = dot(cross, lags[...], 0, 0).astype(low)
    stage3[...] = partial.reshape(stage3.shape)
    for d in range(1, owners):
        j = (mine + d) % owners
        device = at(j // (segs * recs), j // recs % segs, j % recs)
        sends.append(push(stage3.at[j], inbox3.at[mine], send3.at[d - 1], recv3.at[mine], device))
    inbox3[mine] = stage3[mine]
    for d in range(1, owners):
        k = (mine + d) % owners
        arrived(inbox3.at[k], recv3.at[k])
    loads[2].wait()
    loads[3].wait()
    synthetic = inbox3[0].astype(jnp.float32)
    for k in range(1, owners):
        synthetic += inbox3[k].astype(jnp.float32)
    window = mask[pl.ds(r, 1), :].astype(jnp.float32)
    inbox4[mine] = (window * jnp.tanh(synthetic - observed[...])).astype(low)
    for d in range(1, owners):
        j = (mine + d) % owners
        device = at(j // (segs * recs), j // recs % segs, j % recs)
        sends.append(push(inbox4.at[mine], inbox4.at[mine], send4.at[d - 1], recv4.at[mine], device))
    for d in range(1, owners):
        k = (mine + d) % owners
        arrived(inbox4.at[k], recv4.at[k])
    weights = inbox4[...].reshape(count, LAGS)
    adjoint = dot(lags[...], weights, 1, 1).astype(low).astype(jnp.float32)
    g0, g1 = (adjoint[:freqs], adjoint[freqs:])
    a0, a1 = (picked[:freqs, :count], picked[freqs:, :count])
    b0, b1 = (picked[:freqs, count:], picked[freqs:, count:])
    grads = jnp.concatenate(
        [
            jnp.concatenate([g0 * b0 - g1 * b1, g0 * a0 + g1 * a1], axis=1),
            jnp.concatenate([g0 * b1 + g1 * b0, g0 * a1 - g1 * a0], axis=1),
        ],
        axis=0,
    ).astype(low)
    summed = dot(grads, select[...], 1, 1).astype(low)
    for place, k in enumerate(order):
        cut = slice(place * chans, (place + 1) * chans)
        stage5[k] = jnp.concatenate([summed[:freqs, cut], summed[freqs:, cut]], axis=1)
    for d in range(1, bands):
        j = (band + d) % bands
        sends.append(push(stage5.at[j], inbox5.at[band], send5.at[d - 1], recv5.at[band], at_band(j)))
    inbox5[band] = stage5[band]
    loads[4].wait()
    for d in range(1, bands):
        k = (band + d) % bands
        arrived(inbox5.at[k], recv5.at[k])
    held = []
    for parity in range(2):
        pieces = []
        for k in range(parity * bands // 2, (parity + 1) * bands // 2):
            pieces += [inbox5[k][:, :chans], inbox5[k][:, chans:]]
        held.append(jnp.concatenate(pieces, axis=0))
    for h in range(fibres // 2):
        cut = slice(h * span, (h + 1) * span)
        even = dot(backward[0, cut], held[0])
        odd = dot(backward[1, cut], held[1])
        for late, value in enumerate((even + odd, even - odd)):
            value = value.astype(low)
            stage6[h + late * (fibres // 2)] = jnp.concatenate([value[:rows], value[rows:]], axis=1)
    for d in range(1, fibres):
        j = (f + d) % fibres
        sends.append(push(stage6.at[j], inbox6.at[f], send6.at[d - 1], recv6.at[f], at(j, s, r)))
    inbox6[f] = stage6[f]
    for d in range(1, fibres):
        k = (f + d) % fibres
        arrived(inbox6.at[k], recv6.at[k])
    out[:rows, :] = jnp.concatenate([inbox6[k][:, :chans] for k in range(fibres)], axis=1)
    out[rows:, :] = jnp.concatenate([inbox6[k][:, chans:] for k in range(fibres)], axis=1)
    for copy in sends:
        copy.wait_send()


def fused_on_device(mesh_shape, tables, records, pairs, observed, lag_mask):
    fibres, segs, recs = (mesh_shape[name] for name in ("fibre", "seg", "rec"))
    bands = fibres * segs
    owners = bands * recs
    _, span, width = records.shape
    freqs = F // bands
    chans = width // fibres
    count = pairs.shape[0] * BLOCK
    low = jnp.bfloat16
    vmem = pl.BlockSpec(memory_space=pltpu.VMEM)
    hbm = pl.BlockSpec(memory_space=pltpu.HBM)
    row = (freqs, 2 * chans)
    slab = (span // 2, 2 * chans)
    corr = (BLOCK, LAGS)

    def sems(size):
        return [pltpu.SemaphoreType.DMA((size - 1,)), pltpu.SemaphoreType.DMA((size,))]

    result = pl.pallas_call(
        functools.partial(fused_kernel, (fibres, segs, recs)),
        out_shape=jax.ShapeDtypeStruct((span, width), low),
        in_specs=[hbm, pl.BlockSpec(memory_space=pltpu.SMEM)] + [hbm] * 5,
        out_specs=vmem,
        scratch_shapes=[
            pltpu.VMEM((span, width), low),
            pltpu.VMEM(corr, jnp.float32),
            pltpu.VMEM(lag_mask.shape, jnp.int32),
            pltpu.VMEM((2 * F, S // 2), low),
            pltpu.VMEM((2, S // 2, F), low),
            pltpu.VMEM((2 * freqs, LAGS), low),
            pltpu.VMEM((fibres,) + slab, low),
            pltpu.VMEM((fibres,) + slab, low),
            pltpu.VMEM((S, chans), low),
            pltpu.VMEM((bands - 1,) + row, low),
            pltpu.VMEM((bands,) + row, low),
            pltpu.VMEM((2 * freqs, 2 * count), jnp.float32),
            pltpu.VMEM((segs * width, 2 * count), low),
            pltpu.VMEM((owners,) + corr, low),
            pltpu.VMEM((owners,) + corr, low),
            pltpu.VMEM((owners,) + corr, low),
            pltpu.VMEM((bands,) + row, low),
            pltpu.VMEM((bands,) + row, low),
            pltpu.VMEM((fibres,) + slab, low),
            pltpu.VMEM((fibres,) + slab, low),
            pltpu.SemaphoreType.DMA((6,)),
            *sems(fibres), *sems(bands), *sems(owners), *sems(owners), *sems(bands), *sems(fibres),
        ],
        compiler_params=pltpu.CompilerParams(
            has_side_effects=True, vmem_limit_bytes=VMEM_GRANT
        ),
        name="adjoint",
    )(records[0], pairs.T, observed, lag_mask, *tables)
    return result[None]


def fits_fused(shape, records, pairs):
    fibres, segs, recs = (shape[name] for name in ("fibre", "seg", "rec"))
    chans = records.shape[2] // (shape["groups"] * segs * fibres)
    return (
        fibres == 4
        and recs == 2
        and 2 * chans == 128
        and pairs.shape[0] == fibres * segs * recs
        and F // (fibres * segs) >= 16
    )


def solution(mesh):
    in_specs = (
        P("rec", "fibre", ("groups", "seg")),
        P(),
        P(("groups", "fibre", "seg"), None, None),
        P(("groups", "fibre", "seg"), None),
    )
    out_specs = P("rec", "fibre", ("groups", "seg"))
    shape = dict(mesh.shape)

    def run(records, pairs, observed, lag_mask):
        args = (records, pairs, observed, lag_mask)
        if not fits_fused(shape, records, pairs):
            return jax.shard_map(
                on_device, mesh=mesh, in_specs=in_specs, out_specs=out_specs, check_vma=False
            )(*args)
        tables = [jnp.asarray(t) for t in band_tables(shape["fibre"] * shape["seg"])]

        def body(*blocks):
            return fused_on_device(shape, tables, *blocks)

        return jax.shard_map(
            body, mesh=mesh, in_specs=in_specs, out_specs=out_specs, check_vma=False
        )(*args)

    return run
```

```python
import functools

import jax
import jax.numpy as jnp
import numpy as np
from jax import lax
from jax.experimental import pallas as pl
from jax.experimental.pallas import tpu as pltpu
from jax.sharding import PartitionSpec as P

S = 2048
F = 1024
LAGS = 256
BLOCK = 32
CH_DEV = 64
VMEM_GRANT = 67_043_328


def forward_table():
    freq_index = jnp.arange(F, dtype=jnp.int32)
    time_index = jnp.arange(S, dtype=jnp.int32)
    phase = freq_index[:, None] * time_index[None, :] % S
    angles = phase.astype(jnp.float32) * (2.0 * jnp.pi / S)
    scale = 1.0 / jnp.sqrt(jnp.float32(S))
    return jnp.stack(
        [
            (jnp.cos(angles) * scale).astype(jnp.bfloat16),
            (-jnp.sin(angles) * scale).astype(jnp.bfloat16),
        ],
        axis=1,
    )


def lag_table():
    freq_index = jnp.arange(F, dtype=jnp.int32)
    shifts = (jnp.arange(LAGS, dtype=jnp.int32) - LAGS // 2) % S
    phase = freq_index[:, None] * shifts[None, :] % S
    angles = phase.astype(jnp.float32) * (2.0 * jnp.pi / S)
    scale = 1.0 / jnp.sqrt(jnp.float32(F))
    return jnp.stack(
        [
            (jnp.cos(angles) * scale).astype(jnp.bfloat16),
            (-jnp.sin(angles) * scale).astype(jnp.bfloat16),
        ],
        axis=1,
    )


def synthesize(incoming, table):
    count = incoming.shape[-1]
    flat = incoming.reshape(2 * F, count)
    result = jnp.einsum(
        "qn,qt->tn", flat, table.reshape(2 * F, S), preferred_element_type=jnp.float32
    )
    return result.astype(jnp.bfloat16)


def on_device(records, pairs, observed, lag_mask):
    fibre_count = lax.axis_size("fibre")
    seg_count = lax.axis_size("seg")
    spread_count = fibre_count * seg_count
    freq_dev = F // spread_count
    blocks_dev = CH_DEV // BLOCK
    block_count = CH_DEV * spread_count // BLOCK
    pair_total = pairs.shape[0]
    pairs_dev = pair_total // spread_count
    table = forward_table()
    lags = lag_table()
    spans = records.reshape(1, S // fibre_count, fibre_count, CH_DEV)
    incoming = lax.all_to_all(spans, "fibre", split_axis=2, concat_axis=1, tiled=True)
    count = incoming.shape[3]
    signal = incoming.reshape(S, count)
    result = jnp.einsum(
        "qs,sn->qn", table.reshape(2 * F, S), signal, preferred_element_type=jnp.float32
    )
    spectra = result.reshape(F, 2, count).astype(jnp.bfloat16)
    widened = lax.all_to_all(spectra, ("fibre", "seg"), split_axis=0, concat_axis=2, tiled=True)
    seg_blocks = fibre_count * blocks_dev
    slot_ids = (
        pairs % seg_blocks // blocks_dev * seg_count + pairs // seg_blocks
    ) * blocks_dev + pairs % blocks_dev
    blocks_grid = widened.reshape(freq_dev, 2, block_count, BLOCK)
    first_side = jnp.take(blocks_grid, slot_ids[:, 0], axis=2).astype(jnp.float32)
    second_side = jnp.take(blocks_grid, slot_ids[:, 1], axis=2).astype(jnp.float32)
    first_re, first_im = (first_side[:, 0], first_side[:, 1])
    second_re, second_im = (second_side[:, 0], second_side[:, 1])
    cross_re = first_re * second_re + first_im * second_im
    cross_im = first_im * second_re - first_re * second_im
    cross_spec = jnp.stack([cross_re, cross_im], axis=1).astype(jnp.bfloat16)
    cross_spec = cross_spec.reshape(freq_dev, 2, spread_count, pairs_dev * BLOCK)
    owned_spec = lax.all_to_all(
        cross_spec, ("fibre", "seg"), split_axis=2, concat_axis=0, tiled=True
    )
    owned_spec = owned_spec.reshape(F, 2, pairs_dev * BLOCK)
    partial_corr = jnp.einsum("wpx,wpl->xl", owned_spec, lags, preferred_element_type=jnp.float32)
    synthetic = (
        lax.psum(partial_corr.astype(jnp.bfloat16), "rec")
        .astype(jnp.float32)
        .reshape(pairs_dev, BLOCK, LAGS)
    )
    weights = lag_mask[:, None, :].astype(jnp.float32) * jnp.tanh(synthetic - observed)
    weights_low = weights.astype(jnp.bfloat16).reshape(pairs_dev * BLOCK, LAGS)
    adjoint_spec = jnp.einsum("xl,wpl->wpx", weights_low, lags, preferred_element_type=jnp.float32)
    adjoint_spec = adjoint_spec.astype(jnp.bfloat16).reshape(F, 2, 1, pairs_dev * BLOCK)
    returned = lax.all_to_all(
        adjoint_spec, ("fibre", "seg"), split_axis=0, concat_axis=2, tiled=True
    )
    returned = returned.reshape(freq_dev, 2, pair_total, BLOCK).astype(jnp.float32)
    adjoint_re, adjoint_im = (returned[:, 0], returned[:, 1])
    grad_first = jnp.stack(
        [
            adjoint_re * second_re - adjoint_im * second_im,
            adjoint_re * second_im + adjoint_im * second_re,
        ],
        axis=1,
    )
    grad_second = jnp.stack(
        [
            adjoint_re * first_re + adjoint_im * first_im,
            adjoint_re * first_im - adjoint_im * first_re,
        ],
        axis=1,
    )
    contributions = jnp.concatenate([grad_first, grad_second], axis=2)
    endpoint_ids = jnp.concatenate([slot_ids[:, 0], slot_ids[:, 1]])
    summed = jax.ops.segment_sum(
        jnp.moveaxis(contributions, 2, 0), endpoint_ids, num_segments=block_count
    )
    block_adjoint = jnp.moveaxis(summed, 0, 2).astype(jnp.bfloat16)
    outgoing = block_adjoint.reshape(freq_dev, 2, spread_count, CH_DEV)
    sources = synthesize(
        lax.all_to_all(outgoing, ("fibre", "seg"), split_axis=2, concat_axis=0, tiled=True), table
    )
    regrouped = lax.all_to_all(sources, "fibre", split_axis=0, concat_axis=1, tiled=True)
    return regrouped[None]


def angle_parts(freqs, times, scale):
    phase = (freqs[:, None].astype(np.int64) * times[None, :]) % S
    angles = phase.astype(np.float32) * np.float32(2.0 * np.pi / S)
    return np.stack([np.cos(angles) * scale, -np.sin(angles) * scale])


def band_tables(spread_count):
    order = np.concatenate([np.arange(0, F, 2), np.arange(1, F, 2)]).reshape(spread_count, -1)
    half = np.arange(S // 2)
    scale = np.float32(1.0) / np.sqrt(np.float32(S))
    forward = np.concatenate(
        [angle_parts(band, half, scale).reshape(-1, S // 2) for band in order]
    )
    backward = np.stack([forward[:F].T, forward[F:].T])
    shifts = (np.arange(LAGS) - LAGS // 2) % S
    lag_scale = np.float32(1.0) / np.sqrt(np.float32(F))
    lags = np.stack([angle_parts(band, shifts, lag_scale).reshape(-1, LAGS) for band in order])
    return [table.astype(jnp.bfloat16) for table in (forward, backward, lags)]


def dot(left, right, left_dim=1, right_dim=0):
    return lax.dot_general(
        left,
        right,
        (((left_dim,), (right_dim,)), ((), ())),
        preferred_element_type=jnp.float32,
    )


def fused_kernel(
    sizes, x_hbm, pairs, observed_hbm, mask_hbm, forward_hbm, backward_hbm, lags_hbm, out,
    x, observed, mask, forward, backward, lags, stage1, inbox1, signal, stage2, inbox2, picked, select, cross,
    stage_core, inbox_core, stage3, inbox3, inbox4, stage5, inbox5, stage6, inbox6, load_sem,
    core_sem, relay_send, relay_recv,
    send1, recv1, send2, recv2, send3, recv3, send4, recv4, send5, recv5, send6, recv6,
):
    fibres, segs, recs = sizes
    bands = fibres * segs
    g, f, s, r = (lax.axis_index(name) for name in ("groups", "fibre", "seg", "rec"))
    band = f * segs + s
    span, width = x.shape
    rows = span // 2
    chans = width // fibres
    freqs = F // bands
    low = jnp.bfloat16

    def at(fibre, seg, rec):
        return (g, fibre, seg, rec)

    def at_band(index):
        return at(index // segs, index % segs, r)

    def push(src, dst, send, recv, device):
        copy = pltpu.make_async_remote_copy(
            src_ref=src, dst_ref=dst, send_sem=send, recv_sem=recv,
            device_id=device, device_id_type=pl.DeviceIdType.MESH,
        )
        copy.start()
        return copy

    def arrived(dst, recv):
        pltpu.make_async_remote_copy(
            src_ref=dst, dst_ref=dst, send_sem=recv, recv_sem=recv,
            device_id=at(f, s, 1 - r), device_id_type=pl.DeviceIdType.MESH,
        ).wait_recv()

    def flipped(index, bits):
        result, bit = 0, 1
        while bit < bands:
            digit = index // bit % 2
            result += bit * (1 - digit if bits // bit % 2 else digit)
            bit *= 2
        return result

    partner = at(f, s, 1 - r)
    sends = []
    first_load = pltpu.make_async_copy(x_hbm, x, load_sem.at[0])
    first_load.start()
    loads = [
        pltpu.make_async_copy(forward_hbm, forward, load_sem.at[1]),
        pltpu.make_async_copy(lags_hbm.at[band], lags, load_sem.at[2]),
        pltpu.make_async_copy(observed_hbm.at[r], observed, load_sem.at[3]),
        pltpu.make_async_copy(mask_hbm, mask, load_sem.at[4]),
        pltpu.make_async_copy(backward_hbm, backward, load_sem.at[5]),
    ]
    first_load.wait()
    for load in loads:
        load.start()
    for j in range(fibres):
        part = x[:, j * chans : (j + 1) * chans]
        stage1[j] = jnp.concatenate([part[:rows], part[rows:]], axis=1)
    for d in range(fibres - 1, 0, -1):
        j = flipped(f, d)
        sends.append(push(stage1.at[j], inbox1.at[f], send1.at[d - 1], recv1.at[f], at(j, s, r)))
    inbox1[f] = stage1[f]

    total = select.shape[0]
    count = pairs.shape[1] * BLOCK
    lane = lax.broadcasted_iota(jnp.int32, (1, 2 * count), 1)
    target = lane
    for side in range(2):
        for n in range(pairs.shape[1]):
            first = side * count + n * BLOCK
            n = n % bands * recs + n // bands
            inside = (lane >= first) & (lane < first + BLOCK)
            target = jnp.where(inside, lane + (pairs[side, n] * BLOCK - first), target)
    row = lax.broadcasted_iota(jnp.int32, (total, 2 * count), 0)
    select[...] = jnp.where(row == target, 1.0, 0.0).astype(low)

    for d in range(1, fibres):
        k = (f + d) % fibres
        arrived(inbox1.at[k], recv1.at[k])
    for h in range(fibres // 2):
        early = inbox1[h].astype(jnp.float32)
        late = inbox1[h + fibres // 2].astype(jnp.float32)
        for parity, value in enumerate((early + late, early - late)):
            value = value.astype(low)
            base = parity * (S // 2) + h * span
            signal[base : base + rows] = value[:, :chans]
            signal[base + rows : base + span] = value[:, chans:]

    loads[0].wait()
    half = bands // 2
    for far in (1, 0):
        parity = flipped(f, far * (fibres // 2)) // (fibres // 2)
        top = pl.multiple_of(parity * F, F)
        held = signal[pl.ds(pl.multiple_of(parity * (S // 2), S // 2), S // 2), :]
        result = dot(forward[pl.ds(top, F), :], held).astype(low)
        for i in range(half):
            block = result[i * 2 * freqs : (i + 1) * 2 * freqs]
            stage2[parity * half + i] = jnp.concatenate([block[:freqs], block[freqs:]], axis=1)
        for d in range((far + 1) * half - 1, max(far * half - 1, 0), -1):
            j = flipped(band, d)
            sends.append(
                push(stage2.at[j], inbox2.at[band], send2.at[d - 1], recv2.at[band], at_band(j))
            )
    inbox2[band] = stage2[band]
    for d in range(1, bands):
        k = (band + d) % bands
        arrived(inbox2.at[k], recv2.at[k])
    order = [fibre * segs + seg for seg in range(segs) for fibre in range(fibres)]
    spectra = jnp.concatenate(
        [
            jnp.concatenate([inbox2[k][:, p * chans : (p + 1) * chans] for k in order], axis=1)
            for p in range(2)
        ],
        axis=0,
    )
    picked[...] = dot(spectra, select[...])
    share = count // recs
    for h in range(recs):
        a0, a1, b0, b1 = (
            picked[p * freqs : (p + 1) * freqs, side * count + h * share : side * count + (h + 1) * share]
            for side in range(2)
            for p in range(2)
        )
        cross[h] = jnp.concatenate([a0 * b0 + a1 * b1, a1 * b0 - a0 * b1], axis=0).astype(low)
    loads[1].wait()
    stage_core[...] = dot(cross[1 - r], lags[...], 0, 0).astype(low)
    sends.append(push(stage_core, inbox_core, core_sem.at[0], core_sem.at[1], partner))
    partial = dot(cross[r], lags[...], 0, 0)
    arrived(inbox_core, core_sem.at[1])
    partial = (partial + inbox_core[...].astype(jnp.float32)).astype(low)
    stage3[...] = partial.reshape(stage3.shape)
    for d in range(bands - 1, 0, -1):
        j = flipped(band, d)
        sends.append(push(stage3.at[j], inbox3.at[band], send3.at[d - 1], recv3.at[band], at_band(j)))
    inbox3[band] = stage3[band]
    loads[2].wait()
    loads[3].wait()
    for d in range(1, bands):
        k = flipped(band, d)
        arrived(inbox3.at[k], recv3.at[k])
    synthetic = inbox3[0].astype(jnp.float32)
    for k in range(1, bands):
        synthetic += inbox3[k].astype(jnp.float32)
    window = mask[pl.ds(r, 1), :].astype(jnp.float32)
    inbox4[r, band] = (window * jnp.tanh(synthetic - observed[...])).astype(low)
    own = inbox4.at[r, band]
    for d in range(bands - 1, 0, -1):
        j = flipped(band, d)
        sends.append(push(own, own, send4.at[d - 1], recv4.at[band], at_band(j)))
    sends.append(push(own, own, relay_send.at[0], relay_recv.at[band], partner))
    for d in range(1, bands):
        k = flipped(band, d)
        arrived(inbox4.at[r, k], recv4.at[k])
        got = inbox4.at[r, k]
        sends.append(push(got, got, relay_send.at[d], relay_recv.at[k], partner))
    for d in range(bands):
        k = flipped(band, d)
        arrived(inbox4.at[1 - r, k], relay_recv.at[k])
    weights = inbox4[...].reshape(count, LAGS)
    adjoint = dot(lags[...], weights, 1, 1).astype(low).astype(jnp.float32)
    g0, g1 = (adjoint[:freqs], adjoint[freqs:])
    a0, a1 = (picked[:freqs, :count], picked[freqs:, :count])
    b0, b1 = (picked[:freqs, count:], picked[freqs:, count:])
    grads = jnp.concatenate(
        [
            jnp.concatenate([g0 * b0 - g1 * b1, g0 * a0 + g1 * a1], axis=1),
            jnp.concatenate([g0 * b1 + g1 * b0, g0 * a1 - g1 * a0], axis=1),
        ],
        axis=0,
    ).astype(low)
    summed = dot(grads, select[...], 1, 1).astype(low)
    for place, k in enumerate(order):
        cut = slice(place * chans, (place + 1) * chans)
        stage5[k] = jnp.concatenate([summed[:freqs, cut], summed[freqs:, cut]], axis=1)
    for d in range(bands - 1, 0, -1):
        j = flipped(band, d)
        sends.append(push(stage5.at[j], inbox5.at[band], send5.at[d - 1], recv5.at[band], at_band(j)))
    inbox5[band] = stage5[band]
    loads[4].wait()
    for d in range(1, bands):
        k = (band + d) % bands
        arrived(inbox5.at[k], recv5.at[k])
    held = []
    for parity in range(2):
        pieces = []
        for k in range(parity * bands // 2, (parity + 1) * bands // 2):
            pieces += [inbox5[k][:, :chans], inbox5[k][:, chans:]]
        held.append(jnp.concatenate(pieces, axis=0))
    for i in range(1, -1, -1):
        h = flipped(f, i) % 2
        cut = pl.ds(pl.multiple_of(h * span, span), span)
        even = dot(backward[0, cut, :], held[0])
        odd = dot(backward[1, cut, :], held[1])
        for late, value in enumerate((even + odd, even - odd)):
            value = value.astype(low)
            stage6[h + late * 2] = jnp.concatenate([value[:rows], value[rows:]], axis=1)
        for d in (2 + i, i):
            if d > 0:
                j = flipped(f, d)
                sends.append(push(stage6.at[j], inbox6.at[f], send6.at[d - 1], recv6.at[f], at(j, s, r)))
    inbox6[f] = stage6[f]
    for d in range(1, fibres):
        k = (f + d) % fibres
        arrived(inbox6.at[k], recv6.at[k])
    out[:rows, :] = jnp.concatenate([inbox6[k][:, :chans] for k in range(fibres)], axis=1)
    out[rows:, :] = jnp.concatenate([inbox6[k][:, chans:] for k in range(fibres)], axis=1)
    for copy in sends:
        copy.wait_send()


def fused_on_device(mesh_shape, tables, records, pairs, observed, lag_mask):
    fibres, segs, recs = (mesh_shape[name] for name in ("fibre", "seg", "rec"))
    bands = fibres * segs
    _, span, width = records.shape
    freqs = F // bands
    chans = width // fibres
    count = pairs.shape[0] * BLOCK
    low = jnp.bfloat16
    vmem = pl.BlockSpec(memory_space=pltpu.VMEM)
    hbm = pl.BlockSpec(memory_space=pltpu.HBM)
    row = (freqs, 2 * chans)
    slab = (span // 2, 2 * chans)
    corr = (BLOCK, LAGS)

    def sems(size):
        return [pltpu.SemaphoreType.DMA((size - 1,)), pltpu.SemaphoreType.DMA((size,))]

    result = pl.pallas_call(
        functools.partial(fused_kernel, (fibres, segs, recs)),
        out_shape=jax.ShapeDtypeStruct((span, width), low),
        in_specs=[hbm, pl.BlockSpec(memory_space=pltpu.SMEM)] + [hbm] * 5,
        out_specs=vmem,
        scratch_shapes=[
            pltpu.VMEM((span, width), low),
            pltpu.VMEM(corr, jnp.float32),
            pltpu.VMEM(lag_mask.shape, jnp.int32),
            pltpu.VMEM((2 * F, S // 2), low),
            pltpu.VMEM((2, S // 2, F), low),
            pltpu.VMEM((2 * freqs, LAGS), low),
            pltpu.VMEM((fibres,) + slab, low),
            pltpu.VMEM((fibres,) + slab, low),
            pltpu.VMEM((S, chans), low),
            pltpu.VMEM((bands,) + row, low),
            pltpu.VMEM((bands,) + row, low),
            pltpu.VMEM((2 * freqs, 2 * count), jnp.float32),
            pltpu.VMEM((segs * width, 2 * count), low),
            pltpu.VMEM((recs, 2 * freqs, count // recs), low),
            pltpu.VMEM((count // recs, LAGS), low),
            pltpu.VMEM((count // recs, LAGS), low),
            pltpu.VMEM((bands,) + corr, low),
            pltpu.VMEM((bands,) + corr, low),
            pltpu.VMEM((recs, bands) + corr, low),
            pltpu.VMEM((bands,) + row, low),
            pltpu.VMEM((bands,) + row, low),
            pltpu.VMEM((fibres,) + slab, low),
            pltpu.VMEM((fibres,) + slab, low),
            pltpu.SemaphoreType.DMA((6,)),
            pltpu.SemaphoreType.DMA((2,)),
            pltpu.SemaphoreType.DMA((bands,)),
            pltpu.SemaphoreType.DMA((bands,)),
            *sems(fibres), *sems(bands), *sems(bands), *sems(bands), *sems(bands), *sems(fibres),
        ],
        compiler_params=pltpu.CompilerParams(
            has_side_effects=True, vmem_limit_bytes=VMEM_GRANT
        ),
        name="adjoint",
    )(records[0], pairs.T, observed, lag_mask, *tables)
    return result[None]


def fits_fused(shape, records, pairs):
    fibres, segs, recs = (shape[name] for name in ("fibre", "seg", "rec"))
    chans = records.shape[2] // (shape["groups"] * segs * fibres)
    return (
        fibres == 4
        and recs == 2
        and segs & (segs - 1) == 0
        and 2 * chans == 128
        and pairs.shape[0] == fibres * segs * recs
        and F // (fibres * segs) >= 16
    )


def solution(mesh):
    in_specs = (
        P("rec", "fibre", ("groups", "seg")),
        P(),
        P(("groups", "fibre", "seg"), None, None),
        P(("groups", "fibre", "seg"), None),
    )
    out_specs = P("rec", "fibre", ("groups", "seg"))
    shape = dict(mesh.shape)

    def run(records, pairs, observed, lag_mask):
        args = (records, pairs, observed, lag_mask)
        if not fits_fused(shape, records, pairs):
            return jax.shard_map(
                on_device, mesh=mesh, in_specs=in_specs, out_specs=out_specs, check_vma=False
            )(*args)
        tables = [jnp.asarray(t) for t in band_tables(shape["fibre"] * shape["seg"])]

        def body(*blocks):
            return fused_on_device(shape, tables, *blocks)

        return jax.shard_map(
            body, mesh=mesh, in_specs=in_specs, out_specs=out_specs, check_vma=False
        )(*args)

    return run
```

```python
import functools

import jax
import jax.numpy as jnp
import numpy as np
from jax import lax
from jax.experimental import pallas as pl
from jax.experimental.pallas import tpu as pltpu
from jax.sharding import PartitionSpec as P

S = 2048
F = 1024
LAGS = 256
BLOCK = 32
CH_DEV = 64
VMEM_GRANT = 66387968


def forward_table():
    freq_index = jnp.arange(F, dtype=jnp.int32)
    time_index = jnp.arange(S, dtype=jnp.int32)
    phase = freq_index[:, None] * time_index[None, :] % S
    angles = phase.astype(jnp.float32) * (2.0 * jnp.pi / S)
    scale = 1.0 / jnp.sqrt(jnp.float32(S))
    return jnp.stack(
        [
            (jnp.cos(angles) * scale).astype(jnp.bfloat16),
            (-jnp.sin(angles) * scale).astype(jnp.bfloat16),
        ],
        axis=1,
    )


def lag_table():
    freq_index = jnp.arange(F, dtype=jnp.int32)
    shifts = (jnp.arange(LAGS, dtype=jnp.int32) - LAGS // 2) % S
    phase = freq_index[:, None] * shifts[None, :] % S
    angles = phase.astype(jnp.float32) * (2.0 * jnp.pi / S)
    scale = 1.0 / jnp.sqrt(jnp.float32(F))
    return jnp.stack(
        [
            (jnp.cos(angles) * scale).astype(jnp.bfloat16),
            (-jnp.sin(angles) * scale).astype(jnp.bfloat16),
        ],
        axis=1,
    )


def synthesize(incoming, table):
    count = incoming.shape[-1]
    flat = incoming.reshape(2 * F, count)
    result = jnp.einsum(
        "qn,qt->tn", flat, table.reshape(2 * F, S), preferred_element_type=jnp.float32
    )
    return result.astype(jnp.bfloat16)


def on_device(records, pairs, observed, lag_mask):
    fibre_count = lax.axis_size("fibre")
    seg_count = lax.axis_size("seg")
    spread_count = fibre_count * seg_count
    freq_dev = F // spread_count
    blocks_dev = CH_DEV // BLOCK
    block_count = CH_DEV * spread_count // BLOCK
    pair_total = pairs.shape[0]
    pairs_dev = pair_total // spread_count
    table = forward_table()
    lags = lag_table()
    spans = records.reshape(1, S // fibre_count, fibre_count, CH_DEV)
    incoming = lax.all_to_all(spans, "fibre", split_axis=2, concat_axis=1, tiled=True)
    count = incoming.shape[3]
    signal = incoming.reshape(S, count)
    result = jnp.einsum(
        "qs,sn->qn", table.reshape(2 * F, S), signal, preferred_element_type=jnp.float32
    )
    spectra = result.reshape(F, 2, count).astype(jnp.bfloat16)
    widened = lax.all_to_all(spectra, ("fibre", "seg"), split_axis=0, concat_axis=2, tiled=True)
    seg_blocks = fibre_count * blocks_dev
    slot_ids = (
        pairs % seg_blocks // blocks_dev * seg_count + pairs // seg_blocks
    ) * blocks_dev + pairs % blocks_dev
    blocks_grid = widened.reshape(freq_dev, 2, block_count, BLOCK)
    first_side = jnp.take(blocks_grid, slot_ids[:, 0], axis=2).astype(jnp.float32)
    second_side = jnp.take(blocks_grid, slot_ids[:, 1], axis=2).astype(jnp.float32)
    first_re, first_im = (first_side[:, 0], first_side[:, 1])
    second_re, second_im = (second_side[:, 0], second_side[:, 1])
    cross_re = first_re * second_re + first_im * second_im
    cross_im = first_im * second_re - first_re * second_im
    cross_spec = jnp.stack([cross_re, cross_im], axis=1).astype(jnp.bfloat16)
    cross_spec = cross_spec.reshape(freq_dev, 2, spread_count, pairs_dev * BLOCK)
    owned_spec = lax.all_to_all(
        cross_spec, ("fibre", "seg"), split_axis=2, concat_axis=0, tiled=True
    )
    owned_spec = owned_spec.reshape(F, 2, pairs_dev * BLOCK)
    partial_corr = jnp.einsum("wpx,wpl->xl", owned_spec, lags, preferred_element_type=jnp.float32)
    synthetic = (
        lax.psum(partial_corr.astype(jnp.bfloat16), "rec")
        .astype(jnp.float32)
        .reshape(pairs_dev, BLOCK, LAGS)
    )
    weights = lag_mask[:, None, :].astype(jnp.float32) * jnp.tanh(synthetic - observed)
    weights_low = weights.astype(jnp.bfloat16).reshape(pairs_dev * BLOCK, LAGS)
    adjoint_spec = jnp.einsum("xl,wpl->wpx", weights_low, lags, preferred_element_type=jnp.float32)
    adjoint_spec = adjoint_spec.astype(jnp.bfloat16).reshape(F, 2, 1, pairs_dev * BLOCK)
    returned = lax.all_to_all(
        adjoint_spec, ("fibre", "seg"), split_axis=0, concat_axis=2, tiled=True
    )
    returned = returned.reshape(freq_dev, 2, pair_total, BLOCK).astype(jnp.float32)
    adjoint_re, adjoint_im = (returned[:, 0], returned[:, 1])
    grad_first = jnp.stack(
        [
            adjoint_re * second_re - adjoint_im * second_im,
            adjoint_re * second_im + adjoint_im * second_re,
        ],
        axis=1,
    )
    grad_second = jnp.stack(
        [
            adjoint_re * first_re + adjoint_im * first_im,
            adjoint_re * first_im - adjoint_im * first_re,
        ],
        axis=1,
    )
    contributions = jnp.concatenate([grad_first, grad_second], axis=2)
    endpoint_ids = jnp.concatenate([slot_ids[:, 0], slot_ids[:, 1]])
    summed = jax.ops.segment_sum(
        jnp.moveaxis(contributions, 2, 0), endpoint_ids, num_segments=block_count
    )
    block_adjoint = jnp.moveaxis(summed, 0, 2).astype(jnp.bfloat16)
    outgoing = block_adjoint.reshape(freq_dev, 2, spread_count, CH_DEV)
    sources = synthesize(
        lax.all_to_all(outgoing, ("fibre", "seg"), split_axis=2, concat_axis=0, tiled=True), table
    )
    regrouped = lax.all_to_all(sources, "fibre", split_axis=0, concat_axis=1, tiled=True)
    return regrouped[None]


def angle_parts(freqs, times, scale):
    phase = (freqs[:, None].astype(np.int64) * times[None, :]) % S
    angles = phase.astype(np.float32) * np.float32(2.0 * np.pi / S)
    return np.stack([np.cos(angles) * scale, -np.sin(angles) * scale])


def band_tables(spread_count):
    order = np.concatenate([np.arange(0, F, 2), np.arange(1, F, 2)]).reshape(spread_count, -1)
    half = np.arange(S // 2)
    scale = np.float32(1.0) / np.sqrt(np.float32(S))
    forward = np.concatenate(
        [angle_parts(band, half, scale).reshape(-1, S // 2) for band in order]
    )
    backward = np.stack([forward[:F].T, forward[F:].T])
    shifts = (np.arange(LAGS) - LAGS // 2) % S
    lag_scale = np.float32(1.0) / np.sqrt(np.float32(F))
    lags = np.stack([angle_parts(band, shifts, lag_scale).reshape(-1, LAGS) for band in order])
    return [table.astype(jnp.bfloat16) for table in (forward, backward, lags)]


def dot(left, right, left_dim=1, right_dim=0):
    return lax.dot_general(
        left,
        right,
        (((left_dim,), (right_dim,)), ((), ())),
        preferred_element_type=jnp.float32,
    )


def fused_kernel(
    sizes, x_hbm, pairs, observed_hbm, mask_hbm, forward_hbm, backward_hbm, lags_hbm, out,
    x, observed, mask, forward, backward, lags, stage1, inbox1, signal, stage2, inbox2, picked, select, cross,
    stage_core, inbox_core, stage3, inbox3, inbox4, stage5, inbox5, stage6, inbox6, load_sem,
    core_sem, relay_send, relay_recv,
    send1, recv1, send2, recv2, send3, recv3, send4, recv4, send5, recv5, send6, recv6,
):
    fibres, segs, recs = sizes
    bands = fibres * segs
    g, f, s, r = (lax.axis_index(name) for name in ("groups", "fibre", "seg", "rec"))
    band = f * segs + s
    span, width = x.shape
    rows = span // 2
    chans = width // fibres
    freqs = F // bands
    low = jnp.bfloat16

    def at(fibre, seg, rec):
        return (g, fibre, seg, rec)

    def at_band(index):
        return at(index // segs, index % segs, r)

    def push(src, dst, send, recv, device):
        copy = pltpu.make_async_remote_copy(
            src_ref=src, dst_ref=dst, send_sem=send, recv_sem=recv,
            device_id=device, device_id_type=pl.DeviceIdType.MESH,
        )
        copy.start()
        return copy

    def arrived(dst, recv):
        pltpu.make_async_remote_copy(
            src_ref=dst, dst_ref=dst, send_sem=recv, recv_sem=recv,
            device_id=at(f, s, 1 - r), device_id_type=pl.DeviceIdType.MESH,
        ).wait_recv()

    def flipped(index, bits):
        result, bit = 0, 1
        while bit < bands:
            digit = index // bit % 2
            result += bit * (1 - digit if bits // bit % 2 else digit)
            bit *= 2
        return result

    partner = at(f, s, 1 - r)
    barrier = pltpu.get_barrier_semaphore()
    for d in range(1, bands):
        pl.semaphore_signal(
            barrier, inc=1, device_id=at_band(flipped(band, d)), device_id_type=pl.DeviceIdType.MESH
        )
    pl.semaphore_signal(barrier, inc=1, device_id=partner, device_id_type=pl.DeviceIdType.MESH)
    sends = []
    first_load = pltpu.make_async_copy(x_hbm, x, load_sem.at[0])
    first_load.start()
    loads = [
        pltpu.make_async_copy(forward_hbm, forward, load_sem.at[1]),
        pltpu.make_async_copy(lags_hbm.at[band], lags, load_sem.at[2]),
        pltpu.make_async_copy(observed_hbm.at[r], observed, load_sem.at[3]),
        pltpu.make_async_copy(mask_hbm, mask, load_sem.at[4]),
        pltpu.make_async_copy(backward_hbm, backward, load_sem.at[5]),
    ]
    first_load.wait()
    for load in loads:
        load.start()
    for j in range(fibres):
        part = x[:, j * chans : (j + 1) * chans]
        stage1[j] = jnp.concatenate([part[:rows], part[rows:]], axis=1)
    pl.semaphore_wait(barrier, bands)
    for d in range(fibres - 1, 0, -1):
        j = flipped(f, d)
        sends.append(push(stage1.at[j], inbox1.at[f], send1.at[d - 1], recv1.at[f], at(j, s, r)))
    inbox1[f] = stage1[f]

    total = select.shape[0]
    count = pairs.shape[1] * BLOCK
    lane = lax.broadcasted_iota(jnp.int32, (1, 2 * count), 1)
    target = lane
    for side in range(2):
        for n in range(pairs.shape[1]):
            first = side * count + n * BLOCK
            n = n % bands * recs + n // bands
            inside = (lane >= first) & (lane < first + BLOCK)
            target = jnp.where(inside, lane + (pairs[side, n] * BLOCK - first), target)
    row = lax.broadcasted_iota(jnp.int32, (total, 2 * count), 0)
    select[...] = jnp.where(row == target, 1.0, 0.0).astype(low)

    for d in range(1, fibres):
        k = (f + d) % fibres
        arrived(inbox1.at[k], recv1.at[k])
    for h in range(fibres // 2):
        early = inbox1[h].astype(jnp.float32)
        late = inbox1[h + fibres // 2].astype(jnp.float32)
        for parity, value in enumerate((early + late, early - late)):
            value = value.astype(low)
            base = parity * (S // 2) + h * span
            signal[base : base + rows] = value[:, :chans]
            signal[base + rows : base + span] = value[:, chans:]

    loads[0].wait()
    half = bands // 2
    for far in (1, 0):
        parity = flipped(f, far * (fibres // 2)) // (fibres // 2)
        top = pl.multiple_of(parity * F, F)
        held = signal[pl.ds(pl.multiple_of(parity * (S // 2), S // 2), S // 2), :]
        for pair in (1, 0):
            inner = flipped(f % 2, pair)
            start = pl.multiple_of(top + inner * (F // 2), F // 2)
            result = dot(forward[pl.ds(start, F // 2), :], held).astype(low)
            for i in range(segs):
                block = result[i * 2 * freqs : (i + 1) * 2 * freqs]
                stage2[parity * half + inner * segs + i] = jnp.concatenate(
                    [block[:freqs], block[freqs:]], axis=1
                )
            first = far * half + pair * segs
            for d in range(first + segs - 1, max(first - 1, 0), -1):
                j = flipped(band, d)
                sends.append(
                    push(stage2.at[j], inbox2.at[band], send2.at[d - 1], recv2.at[band], at_band(j))
                )
    inbox2[band] = stage2[band]
    for d in range(1, bands):
        k = (band + d) % bands
        arrived(inbox2.at[k], recv2.at[k])
    order = [fibre * segs + seg for seg in range(segs) for fibre in range(fibres)]
    spectra = jnp.concatenate(
        [
            jnp.concatenate([inbox2[k][:, p * chans : (p + 1) * chans] for k in order], axis=1)
            for p in range(2)
        ],
        axis=0,
    )
    picked[...] = dot(spectra, select[...])
    share = count // recs
    for h in range(recs):
        a0, a1, b0, b1 = (
            picked[p * freqs : (p + 1) * freqs, side * count + h * share : side * count + (h + 1) * share]
            for side in range(2)
            for p in range(2)
        )
        cross[h] = jnp.concatenate([a0 * b0 + a1 * b1, a1 * b0 - a0 * b1], axis=0).astype(low)
    loads[1].wait()
    stage_core[...] = dot(cross[1 - r], lags[...], 0, 0).astype(low)
    sends.append(push(stage_core, inbox_core, core_sem.at[0], core_sem.at[1], partner))
    partial = dot(cross[r], lags[...], 0, 0)
    arrived(inbox_core, core_sem.at[1])
    partial = (partial + inbox_core[...].astype(jnp.float32)).astype(low)
    stage3[...] = partial.reshape(stage3.shape)
    for d in range(bands - 1, 0, -1):
        j = flipped(band, d)
        sends.append(push(stage3.at[j], inbox3.at[band], send3.at[d - 1], recv3.at[band], at_band(j)))
    inbox3[band] = stage3[band]
    loads[2].wait()
    loads[3].wait()
    for d in range(1, bands):
        k = flipped(band, d)
        arrived(inbox3.at[k], recv3.at[k])
    synthetic = inbox3[0].astype(jnp.float32)
    for k in range(1, bands):
        synthetic += inbox3[k].astype(jnp.float32)
    window = mask[pl.ds(r, 1), :].astype(jnp.float32)
    inbox4[r, band] = (window * jnp.tanh(synthetic - observed[...])).astype(low)
    own = inbox4.at[r, band]
    for d in range(bands - 1, 0, -1):
        j = flipped(band, d)
        sends.append(push(own, own, send4.at[d - 1], recv4.at[band], at_band(j)))
    sends.append(push(own, own, relay_send.at[0], relay_recv.at[band], partner))
    for d in range(1, bands):
        k = flipped(band, d)
        arrived(inbox4.at[r, k], recv4.at[k])
        got = inbox4.at[r, k]
        sends.append(push(got, got, relay_send.at[d], relay_recv.at[k], partner))
    for d in range(bands):
        k = flipped(band, d)
        arrived(inbox4.at[1 - r, k], relay_recv.at[k])
    weights = inbox4[...].reshape(count, LAGS)
    adjoint = dot(lags[...], weights, 1, 1).astype(low).astype(jnp.float32)
    g0, g1 = (adjoint[:freqs], adjoint[freqs:])
    a0, a1 = (picked[:freqs, :count], picked[freqs:, :count])
    b0, b1 = (picked[:freqs, count:], picked[freqs:, count:])
    grads = jnp.concatenate(
        [
            jnp.concatenate([g0 * b0 - g1 * b1, g0 * a0 + g1 * a1], axis=1),
            jnp.concatenate([g0 * b1 + g1 * b0, g0 * a1 - g1 * a0], axis=1),
        ],
        axis=0,
    ).astype(low)
    summed = dot(grads, select[...], 1, 1).astype(low)
    for place, k in enumerate(order):
        cut = slice(place * chans, (place + 1) * chans)
        stage5[k] = jnp.concatenate([summed[:freqs, cut], summed[freqs:, cut]], axis=1)
    for d in range(bands - 1, 0, -1):
        j = flipped(band, d)
        sends.append(push(stage5.at[j], inbox5.at[band], send5.at[d - 1], recv5.at[band], at_band(j)))
    inbox5[band] = stage5[band]
    loads[4].wait()
    for d in range(1, bands):
        k = (band + d) % bands
        arrived(inbox5.at[k], recv5.at[k])
    held = []
    for parity in range(2):
        pieces = []
        for k in range(parity * bands // 2, (parity + 1) * bands // 2):
            pieces += [inbox5[k][:, :chans], inbox5[k][:, chans:]]
        held.append(jnp.concatenate(pieces, axis=0))
    for i in range(1, -1, -1):
        h = flipped(f, i) % 2
        cut = pl.ds(pl.multiple_of(h * span, span), span)
        even = dot(backward[0, cut, :], held[0])
        odd = dot(backward[1, cut, :], held[1])
        for late, value in enumerate((even + odd, even - odd)):
            value = value.astype(low)
            stage6[h + late * 2] = jnp.concatenate([value[:rows], value[rows:]], axis=1)
        for d in (2 + i, i):
            if d > 0:
                j = flipped(f, d)
                sends.append(push(stage6.at[j], inbox6.at[f], send6.at[d - 1], recv6.at[f], at(j, s, r)))
    inbox6[f] = stage6[f]
    for d in range(1, fibres):
        k = (f + d) % fibres
        arrived(inbox6.at[k], recv6.at[k])
    out[:rows, :] = jnp.concatenate([inbox6[k][:, :chans] for k in range(fibres)], axis=1)
    out[rows:, :] = jnp.concatenate([inbox6[k][:, chans:] for k in range(fibres)], axis=1)
    for copy in sends:
        copy.wait_send()


def fused_on_device(mesh_shape, tables, records, pairs, observed, lag_mask):
    fibres, segs, recs = (mesh_shape[name] for name in ("fibre", "seg", "rec"))
    bands = fibres * segs
    _, span, width = records.shape
    freqs = F // bands
    chans = width // fibres
    count = pairs.shape[0] * BLOCK
    low = jnp.bfloat16
    vmem = pl.BlockSpec(memory_space=pltpu.VMEM)
    hbm = pl.BlockSpec(memory_space=pltpu.HBM)
    row = (freqs, 2 * chans)
    slab = (span // 2, 2 * chans)
    corr = (BLOCK, LAGS)

    def sems(size):
        return [pltpu.SemaphoreType.DMA((size - 1,)), pltpu.SemaphoreType.DMA((size,))]

    result = pl.pallas_call(
        functools.partial(fused_kernel, (fibres, segs, recs)),
        out_shape=jax.ShapeDtypeStruct((span, width), low),
        in_specs=[hbm, pl.BlockSpec(memory_space=pltpu.SMEM)] + [hbm] * 5,
        out_specs=vmem,
        scratch_shapes=[
            pltpu.VMEM((span, width), low),
            pltpu.VMEM(corr, jnp.float32),
            pltpu.VMEM(lag_mask.shape, jnp.int32),
            pltpu.VMEM((2 * F, S // 2), low),
            pltpu.VMEM((2, S // 2, F), low),
            pltpu.VMEM((2 * freqs, LAGS), low),
            pltpu.VMEM((fibres,) + slab, low),
            pltpu.VMEM((fibres,) + slab, low),
            pltpu.VMEM((S, chans), low),
            pltpu.VMEM((bands,) + row, low),
            pltpu.VMEM((bands,) + row, low),
            pltpu.VMEM((2 * freqs, 2 * count), jnp.float32),
            pltpu.VMEM((segs * width, 2 * count), low),
            pltpu.VMEM((recs, 2 * freqs, count // recs), low),
            pltpu.VMEM((count // recs, LAGS), low),
            pltpu.VMEM((count // recs, LAGS), low),
            pltpu.VMEM((bands,) + corr, low),
            pltpu.VMEM((bands,) + corr, low),
            pltpu.VMEM((recs, bands) + corr, low),
            pltpu.VMEM((bands,) + row, low),
            pltpu.VMEM((bands,) + row, low),
            pltpu.VMEM((fibres,) + slab, low),
            pltpu.VMEM((fibres,) + slab, low),
            pltpu.SemaphoreType.DMA((6,)),
            pltpu.SemaphoreType.DMA((2,)),
            pltpu.SemaphoreType.DMA((bands,)),
            pltpu.SemaphoreType.DMA((bands,)),
            *sems(fibres), *sems(bands), *sems(bands), *sems(bands), *sems(bands), *sems(fibres),
        ],
        compiler_params=pltpu.CompilerParams(
            has_side_effects=True, collective_id=0, vmem_limit_bytes=VMEM_GRANT
        ),
        name="adjoint",
    )(records[0], pairs.T, observed, lag_mask, *tables)
    return result[None]


def fits_fused(shape, records, pairs):
    fibres, segs, recs = (shape[name] for name in ("fibre", "seg", "rec"))
    chans = records.shape[2] // (shape["groups"] * segs * fibres)
    return (
        fibres == 4
        and recs == 2
        and segs & (segs - 1) == 0
        and 2 * chans == 128
        and pairs.shape[0] == fibres * segs * recs
        and F // (fibres * segs) >= 16
    )


def solution(mesh):
    in_specs = (
        P("rec", "fibre", ("groups", "seg")),
        P(),
        P(("groups", "fibre", "seg"), None, None),
        P(("groups", "fibre", "seg"), None),
    )
    out_specs = P("rec", "fibre", ("groups", "seg"))
    shape = dict(mesh.shape)

    def run(records, pairs, observed, lag_mask):
        args = (records, pairs, observed, lag_mask)
        if not fits_fused(shape, records, pairs):
            return jax.shard_map(
                on_device, mesh=mesh, in_specs=in_specs, out_specs=out_specs, check_vma=False
            )(*args)
        tables = [jnp.asarray(t) for t in band_tables(shape["fibre"] * shape["seg"])]

        def body(*blocks):
            return fused_on_device(shape, tables, *blocks)

        return jax.shard_map(
            body, mesh=mesh, in_specs=in_specs, out_specs=out_specs, check_vma=False
        )(*args)

    return run
```

```python
import functools

import jax
import jax.numpy as jnp
import numpy as np
from jax import lax
from jax.experimental import pallas as pl
from jax.experimental.pallas import tpu as pltpu
from jax.sharding import PartitionSpec as P

S = 2048
F = 1024
LAGS = 256
BLOCK = 32
CH_DEV = 64
VMEM_GRANT = 60899328


def forward_table():
    freq_index = jnp.arange(F, dtype=jnp.int32)
    time_index = jnp.arange(S, dtype=jnp.int32)
    phase = freq_index[:, None] * time_index[None, :] % S
    angles = phase.astype(jnp.float32) * (2.0 * jnp.pi / S)
    scale = 1.0 / jnp.sqrt(jnp.float32(S))
    return jnp.stack(
        [
            (jnp.cos(angles) * scale).astype(jnp.bfloat16),
            (-jnp.sin(angles) * scale).astype(jnp.bfloat16),
        ],
        axis=1,
    )


def lag_table():
    freq_index = jnp.arange(F, dtype=jnp.int32)
    shifts = (jnp.arange(LAGS, dtype=jnp.int32) - LAGS // 2) % S
    phase = freq_index[:, None] * shifts[None, :] % S
    angles = phase.astype(jnp.float32) * (2.0 * jnp.pi / S)
    scale = 1.0 / jnp.sqrt(jnp.float32(F))
    return jnp.stack(
        [
            (jnp.cos(angles) * scale).astype(jnp.bfloat16),
            (-jnp.sin(angles) * scale).astype(jnp.bfloat16),
        ],
        axis=1,
    )


def synthesize(incoming, table):
    count = incoming.shape[-1]
    flat = incoming.reshape(2 * F, count)
    result = jnp.einsum(
        "qn,qt->tn", flat, table.reshape(2 * F, S), preferred_element_type=jnp.float32
    )
    return result.astype(jnp.bfloat16)


def on_device(records, pairs, observed, lag_mask):
    fibre_count = lax.axis_size("fibre")
    seg_count = lax.axis_size("seg")
    spread_count = fibre_count * seg_count
    freq_dev = F // spread_count
    blocks_dev = CH_DEV // BLOCK
    block_count = CH_DEV * spread_count // BLOCK
    pair_total = pairs.shape[0]
    pairs_dev = pair_total // spread_count
    table = forward_table()
    lags = lag_table()
    spans = records.reshape(1, S // fibre_count, fibre_count, CH_DEV)
    incoming = lax.all_to_all(spans, "fibre", split_axis=2, concat_axis=1, tiled=True)
    count = incoming.shape[3]
    signal = incoming.reshape(S, count)
    result = jnp.einsum(
        "qs,sn->qn", table.reshape(2 * F, S), signal, preferred_element_type=jnp.float32
    )
    spectra = result.reshape(F, 2, count).astype(jnp.bfloat16)
    widened = lax.all_to_all(spectra, ("fibre", "seg"), split_axis=0, concat_axis=2, tiled=True)
    seg_blocks = fibre_count * blocks_dev
    slot_ids = (
        pairs % seg_blocks // blocks_dev * seg_count + pairs // seg_blocks
    ) * blocks_dev + pairs % blocks_dev
    blocks_grid = widened.reshape(freq_dev, 2, block_count, BLOCK)
    first_side = jnp.take(blocks_grid, slot_ids[:, 0], axis=2).astype(jnp.float32)
    second_side = jnp.take(blocks_grid, slot_ids[:, 1], axis=2).astype(jnp.float32)
    first_re, first_im = (first_side[:, 0], first_side[:, 1])
    second_re, second_im = (second_side[:, 0], second_side[:, 1])
    cross_re = first_re * second_re + first_im * second_im
    cross_im = first_im * second_re - first_re * second_im
    cross_spec = jnp.stack([cross_re, cross_im], axis=1).astype(jnp.bfloat16)
    cross_spec = cross_spec.reshape(freq_dev, 2, spread_count, pairs_dev * BLOCK)
    owned_spec = lax.all_to_all(
        cross_spec, ("fibre", "seg"), split_axis=2, concat_axis=0, tiled=True
    )
    owned_spec = owned_spec.reshape(F, 2, pairs_dev * BLOCK)
    partial_corr = jnp.einsum("wpx,wpl->xl", owned_spec, lags, preferred_element_type=jnp.float32)
    synthetic = (
        lax.psum(partial_corr.astype(jnp.bfloat16), "rec")
        .astype(jnp.float32)
        .reshape(pairs_dev, BLOCK, LAGS)
    )
    weights = lag_mask[:, None, :].astype(jnp.float32) * jnp.tanh(synthetic - observed)
    weights_low = weights.astype(jnp.bfloat16).reshape(pairs_dev * BLOCK, LAGS)
    adjoint_spec = jnp.einsum("xl,wpl->wpx", weights_low, lags, preferred_element_type=jnp.float32)
    adjoint_spec = adjoint_spec.astype(jnp.bfloat16).reshape(F, 2, 1, pairs_dev * BLOCK)
    returned = lax.all_to_all(
        adjoint_spec, ("fibre", "seg"), split_axis=0, concat_axis=2, tiled=True
    )
    returned = returned.reshape(freq_dev, 2, pair_total, BLOCK).astype(jnp.float32)
    adjoint_re, adjoint_im = (returned[:, 0], returned[:, 1])
    grad_first = jnp.stack(
        [
            adjoint_re * second_re - adjoint_im * second_im,
            adjoint_re * second_im + adjoint_im * second_re,
        ],
        axis=1,
    )
    grad_second = jnp.stack(
        [
            adjoint_re * first_re + adjoint_im * first_im,
            adjoint_re * first_im - adjoint_im * first_re,
        ],
        axis=1,
    )
    contributions = jnp.concatenate([grad_first, grad_second], axis=2)
    endpoint_ids = jnp.concatenate([slot_ids[:, 0], slot_ids[:, 1]])
    summed = jax.ops.segment_sum(
        jnp.moveaxis(contributions, 2, 0), endpoint_ids, num_segments=block_count
    )
    block_adjoint = jnp.moveaxis(summed, 0, 2).astype(jnp.bfloat16)
    outgoing = block_adjoint.reshape(freq_dev, 2, spread_count, CH_DEV)
    sources = synthesize(
        lax.all_to_all(outgoing, ("fibre", "seg"), split_axis=2, concat_axis=0, tiled=True), table
    )
    regrouped = lax.all_to_all(sources, "fibre", split_axis=0, concat_axis=1, tiled=True)
    return regrouped[None]


def angle_parts(freqs, times, scale):
    phase = (freqs[:, None].astype(np.int64) * times[None, :]) % S
    angles = phase.astype(np.float32) * np.float32(2.0 * np.pi / S)
    return np.stack([np.cos(angles) * scale, -np.sin(angles) * scale])


def band_tables(spread_count):
    order = np.concatenate([np.arange(0, F, 2), np.arange(1, F, 2)]).reshape(spread_count, -1)
    half = np.arange(S // 2)
    scale = np.float32(1.0) / np.sqrt(np.float32(S))
    forward = np.concatenate(
        [angle_parts(band, half, scale).reshape(-1, S // 2) for band in order]
    )
    backward = np.stack([forward[:F].T, forward[F:].T])
    shifts = (np.arange(LAGS) - LAGS // 2) % S
    lag_scale = np.float32(1.0) / np.sqrt(np.float32(F))
    lags = np.stack([angle_parts(band, shifts, lag_scale).reshape(-1, LAGS) for band in order])
    return [table.astype(jnp.bfloat16) for table in (forward, backward, lags)]


def dot(left, right, left_dim=1, right_dim=0):
    return lax.dot_general(
        left,
        right,
        (((left_dim,), (right_dim,)), ((), ())),
        preferred_element_type=jnp.float32,
    )


def fused_kernel(
    sizes, x_hbm, pairs, observed_hbm, mask_hbm, forward_hbm, backward_hbm, lags_hbm, out,
    x, observed, mask, forward, backward, lags, stage1, inbox1, signal, stage2, inbox2, picked, select, cross,
    stage_core, inbox_core, stage3, inbox3, inbox4, stage5, inbox5, stage6, inbox6, load_sem,
    core_sem, relay_send, relay_recv,
    send1, recv1, send2, recv2, send3, recv3, send4, recv4, send5, recv5, send6, recv6,
):
    fibres, segs, recs = sizes
    bands = fibres * segs
    g, f, s, r = (lax.axis_index(name) for name in ("groups", "fibre", "seg", "rec"))
    band = f * segs + s
    span, width = x.shape
    rows = span // 2
    chans = width // fibres
    freqs = F // bands
    low = jnp.bfloat16

    def at(fibre, seg, rec):
        return (g, fibre, seg, rec)

    def at_band(index):
        return at(index // segs, index % segs, r)

    def push(src, dst, send, recv, device):
        copy = pltpu.make_async_remote_copy(
            src_ref=src, dst_ref=dst, send_sem=send, recv_sem=recv,
            device_id=device, device_id_type=pl.DeviceIdType.MESH,
        )
        copy.start()
        return copy

    def arrived(dst, recv):
        pltpu.make_async_remote_copy(
            src_ref=dst, dst_ref=dst, send_sem=recv, recv_sem=recv,
            device_id=at(f, s, 1 - r), device_id_type=pl.DeviceIdType.MESH,
        ).wait_recv()

    def flipped(index, bits):
        result, bit = 0, 1
        while bit < bands:
            digit = index // bit % 2
            result += bit * (1 - digit if bits // bit % 2 else digit)
            bit *= 2
        return result

    partner = at(f, s, 1 - r)
    barrier = pltpu.get_barrier_semaphore()
    for d in range(1, bands):
        pl.semaphore_signal(
            barrier, inc=1, device_id=at_band(flipped(band, d)), device_id_type=pl.DeviceIdType.MESH
        )
    pl.semaphore_signal(barrier, inc=1, device_id=partner, device_id_type=pl.DeviceIdType.MESH)
    sends = []
    first_load = pltpu.make_async_copy(x_hbm, x, load_sem.at[0])
    first_load.start()
    loads = [
        pltpu.make_async_copy(forward_hbm, forward, load_sem.at[1]),
        pltpu.make_async_copy(lags_hbm.at[band], lags, load_sem.at[2]),
        pltpu.make_async_copy(observed_hbm.at[r], observed, load_sem.at[3]),
        pltpu.make_async_copy(mask_hbm, mask, load_sem.at[4]),
        pltpu.make_async_copy(backward_hbm, backward, load_sem.at[5]),
    ]
    first_load.wait()
    for load in loads:
        load.start()
    for j in range(fibres):
        part = x[:, j * chans : (j + 1) * chans]
        stage1[j] = jnp.concatenate([part[:rows], part[rows:]], axis=1)
    pl.semaphore_wait(barrier, bands)
    for d in range(fibres - 1, 0, -1):
        j = flipped(f, d)
        sends.append(push(stage1.at[j], inbox1.at[f], send1.at[d - 1], recv1.at[f], at(j, s, r)))
    inbox1[f] = stage1[f]

    total = select.shape[0]
    count = pairs.shape[1] * BLOCK
    lane = lax.broadcasted_iota(jnp.int32, (1, 2 * count), 1)
    target = lane
    for side in range(2):
        for n in range(pairs.shape[1]):
            first = side * count + n * BLOCK
            n = n % bands * recs + n // bands
            inside = (lane >= first) & (lane < first + BLOCK)
            target = jnp.where(inside, lane + (pairs[side, n] * BLOCK - first), target)
    row = lax.broadcasted_iota(jnp.int32, (total, 2 * count), 0)
    select[...] = jnp.where(row == target, 1.0, 0.0).astype(low)

    for d in range(1, fibres):
        k = (f + d) % fibres
        arrived(inbox1.at[k], recv1.at[k])
    for h in range(fibres // 2):
        early = inbox1[h].astype(jnp.float32)
        late = inbox1[h + fibres // 2].astype(jnp.float32)
        for parity, value in enumerate((early + late, early - late)):
            value = value.astype(low)
            base = parity * (S // 2) + h * span
            signal[base : base + rows] = value[:, :chans]
            signal[base + rows : base + span] = value[:, chans:]

    loads[0].wait()
    half = bands // 2
    for far in (1, 0):
        parity = flipped(f, far * (fibres // 2)) // (fibres // 2)
        top = pl.multiple_of(parity * F, F)
        held = signal[pl.ds(pl.multiple_of(parity * (S // 2), S // 2), S // 2), :]
        for pair in (1, 0):
            inner = flipped(f % 2, pair)
            start = pl.multiple_of(top + inner * (F // 2), F // 2)
            result = dot(forward[pl.ds(start, F // 2), :], held).astype(low)
            for i in range(segs):
                block = result[i * 2 * freqs : (i + 1) * 2 * freqs]
                stage2[parity * half + inner * segs + i] = jnp.concatenate(
                    [block[:freqs], block[freqs:]], axis=1
                )
            first = far * half + pair * segs
            for d in range(first + segs - 1, max(first - 1, 0), -1):
                j = flipped(band, d)
                sends.append(
                    push(stage2.at[j], inbox2.at[band], send2.at[d - 1], recv2.at[band], at_band(j))
                )
    inbox2[band] = stage2[band]
    for d in range(1, bands):
        k = (band + d) % bands
        arrived(inbox2.at[k], recv2.at[k])
    order = [fibre * segs + seg for seg in range(segs) for fibre in range(fibres)]
    spectra = jnp.concatenate(
        [
            jnp.concatenate([inbox2[k][:, p * chans : (p + 1) * chans] for k in order], axis=1)
            for p in range(2)
        ],
        axis=0,
    )
    picked[...] = dot(spectra, select[...])
    share = count // recs
    for h in range(recs):
        a0, a1, b0, b1 = (
            picked[p * freqs : (p + 1) * freqs, side * count + h * share : side * count + (h + 1) * share]
            for side in range(2)
            for p in range(2)
        )
        cross[h] = jnp.concatenate([a0 * b0 + a1 * b1, a1 * b0 - a0 * b1], axis=0).astype(low)
    loads[1].wait()
    stage_core[...] = dot(cross[1 - r], lags[...], 0, 0).astype(low)
    sends.append(push(stage_core, inbox_core, core_sem.at[0], core_sem.at[1], partner))
    partial = dot(cross[r], lags[...], 0, 0)
    arrived(inbox_core, core_sem.at[1])
    partial = (partial + inbox_core[...].astype(jnp.float32)).astype(low)
    stage3[...] = partial.reshape(stage3.shape)
    for d in range(bands - 1, 0, -1):
        j = flipped(band, d)
        sends.append(push(stage3.at[j], inbox3.at[band], send3.at[d - 1], recv3.at[band], at_band(j)))
    inbox3[band] = stage3[band]
    loads[2].wait()
    loads[3].wait()
    for d in range(1, bands):
        k = flipped(band, d)
        arrived(inbox3.at[k], recv3.at[k])
    synthetic = inbox3[0].astype(jnp.float32)
    for k in range(1, bands):
        synthetic += inbox3[k].astype(jnp.float32)
    window = mask[pl.ds(r, 1), :].astype(jnp.float32)
    inbox4[r, band] = (window * jnp.tanh(synthetic - observed[...])).astype(low)
    own = inbox4.at[r, band]
    for d in range(bands - 1, 0, -1):
        j = flipped(band, d)
        sends.append(push(own, own, send4.at[d - 1], recv4.at[band], at_band(j)))
    sends.append(push(own, own, relay_send.at[0], relay_recv.at[band], partner))
    for d in range(1, bands):
        k = flipped(band, d)
        arrived(inbox4.at[r, k], recv4.at[k])
        got = inbox4.at[r, k]
        sends.append(push(got, got, relay_send.at[d], relay_recv.at[k], partner))
    for d in range(bands):
        k = flipped(band, d)
        arrived(inbox4.at[1 - r, k], relay_recv.at[k])
    weights = inbox4[...].reshape(count, LAGS)
    adjoint = dot(lags[...], weights, 1, 1).astype(low).astype(jnp.float32)
    g0, g1 = (adjoint[:freqs], adjoint[freqs:])
    a0, a1 = (picked[:freqs, :count], picked[freqs:, :count])
    b0, b1 = (picked[:freqs, count:], picked[freqs:, count:])
    grads = jnp.concatenate(
        [
            jnp.concatenate([g0 * b0 - g1 * b1, g0 * a0 + g1 * a1], axis=1),
            jnp.concatenate([g0 * b1 + g1 * b0, g0 * a1 - g1 * a0], axis=1),
        ],
        axis=0,
    ).astype(low)
    summed = dot(grads, select[...], 1, 1).astype(low)
    for place, k in enumerate(order):
        cut = slice(place * chans, (place + 1) * chans)
        stage5[k] = jnp.concatenate([summed[:freqs, cut], summed[freqs:, cut]], axis=1)
    for d in range(bands - 1, 0, -1):
        j = flipped(band, d)
        sends.append(push(stage5.at[j], inbox5.at[band], send5.at[d - 1], recv5.at[band], at_band(j)))
    inbox5[band] = stage5[band]
    loads[4].wait()
    for d in range(1, bands):
        k = (band + d) % bands
        arrived(inbox5.at[k], recv5.at[k])
    held = []
    for parity in range(2):
        pieces = []
        for k in range(parity * bands // 2, (parity + 1) * bands // 2):
            pieces += [inbox5[k][:, :chans], inbox5[k][:, chans:]]
        held.append(jnp.concatenate(pieces, axis=0))
    for i in range(1, -1, -1):
        h = flipped(f, i) % 2
        cut = pl.ds(pl.multiple_of(h * span, span), span)
        even = dot(backward[0, cut, :], held[0])
        odd = dot(backward[1, cut, :], held[1])
        for late, value in enumerate((even + odd, even - odd)):
            value = value.astype(low)
            stage6[h + late * 2] = jnp.concatenate([value[:rows], value[rows:]], axis=1)
        for d in (2 + i, i):
            if d > 0:
                j = flipped(f, d)
                sends.append(push(stage6.at[j], inbox6.at[f], send6.at[d - 1], recv6.at[f], at(j, s, r)))
    inbox6[f] = stage6[f]
    for d in range(1, fibres):
        k = (f + d) % fibres
        arrived(inbox6.at[k], recv6.at[k])
    out[:rows, :] = jnp.concatenate([inbox6[k][:, :chans] for k in range(fibres)], axis=1)
    out[rows:, :] = jnp.concatenate([inbox6[k][:, chans:] for k in range(fibres)], axis=1)
    for copy in sends:
        copy.wait_send()


def fused_on_device(mesh_shape, tables, records, pairs, observed, lag_mask):
    fibres, segs, recs = (mesh_shape[name] for name in ("fibre", "seg", "rec"))
    bands = fibres * segs
    _, span, width = records.shape
    freqs = F // bands
    chans = width // fibres
    count = pairs.shape[0] * BLOCK
    low = jnp.bfloat16
    vmem = pl.BlockSpec(memory_space=pltpu.VMEM)
    hbm = pl.BlockSpec(memory_space=pltpu.HBM)
    row = (freqs, 2 * chans)
    slab = (span // 2, 2 * chans)
    corr = (BLOCK, LAGS)

    def sems(size):
        return [pltpu.SemaphoreType.DMA((size - 1,)), pltpu.SemaphoreType.DMA((size,))]

    result = pl.pallas_call(
        functools.partial(fused_kernel, (fibres, segs, recs)),
        out_shape=pltpu.VMEM((span, width), low),
        in_specs=[hbm, pl.BlockSpec(memory_space=pltpu.SMEM)] + [hbm] * 5,
        out_specs=vmem,
        scratch_shapes=[
            pltpu.VMEM((span, width), low),
            pltpu.VMEM(corr, jnp.float32),
            pltpu.VMEM(lag_mask.shape, jnp.int32),
            pltpu.VMEM((2 * F, S // 2), low),
            pltpu.VMEM((2, S // 2, F), low),
            pltpu.VMEM((2 * freqs, LAGS), low),
            pltpu.VMEM((fibres,) + slab, low),
            pltpu.VMEM((fibres,) + slab, low),
            pltpu.VMEM((S, chans), low),
            pltpu.VMEM((bands,) + row, low),
            pltpu.VMEM((bands,) + row, low),
            pltpu.VMEM((2 * freqs, 2 * count), jnp.float32),
            pltpu.VMEM((segs * width, 2 * count), low),
            pltpu.VMEM((recs, 2 * freqs, count // recs), low),
            pltpu.VMEM((count // recs, LAGS), low),
            pltpu.VMEM((count // recs, LAGS), low),
            pltpu.VMEM((bands,) + corr, low),
            pltpu.VMEM((bands,) + corr, low),
            pltpu.VMEM((recs, bands) + corr, low),
            pltpu.VMEM((bands,) + row, low),
            pltpu.VMEM((bands,) + row, low),
            pltpu.VMEM((fibres,) + slab, low),
            pltpu.VMEM((fibres,) + slab, low),
            pltpu.SemaphoreType.DMA((6,)),
            pltpu.SemaphoreType.DMA((2,)),
            pltpu.SemaphoreType.DMA((bands,)),
            pltpu.SemaphoreType.DMA((bands,)),
            *sems(fibres), *sems(bands), *sems(bands), *sems(bands), *sems(bands), *sems(fibres),
        ],
        compiler_params=pltpu.CompilerParams(
            has_side_effects=True, collective_id=0, vmem_limit_bytes=VMEM_GRANT
        ),
        name="adjoint",
    )(records[0], pairs.T, observed, lag_mask, *tables)
    return result[None]


def fits_fused(shape, records, pairs):
    fibres, segs, recs = (shape[name] for name in ("fibre", "seg", "rec"))
    chans = records.shape[2] // (shape["groups"] * segs * fibres)
    return (
        fibres == 4
        and recs == 2
        and segs & (segs - 1) == 0
        and 2 * chans == 128
        and pairs.shape[0] == fibres * segs * recs
        and F // (fibres * segs) >= 16
    )


def solution(mesh):
    in_specs = (
        P("rec", "fibre", ("groups", "seg")),
        P(),
        P(("groups", "fibre", "seg"), None, None),
        P(("groups", "fibre", "seg"), None),
    )
    out_specs = P("rec", "fibre", ("groups", "seg"))
    shape = dict(mesh.shape)

    def run(records, pairs, observed, lag_mask):
        args = (records, pairs, observed, lag_mask)
        if not fits_fused(shape, records, pairs):
            return jax.shard_map(
                on_device, mesh=mesh, in_specs=in_specs, out_specs=out_specs, check_vma=False
            )(*args)
        tables = [jnp.asarray(t) for t in band_tables(shape["fibre"] * shape["seg"])]

        def body(*blocks):
            return fused_on_device(shape, tables, *blocks)

        return jax.shard_map(
            body, mesh=mesh, in_specs=in_specs, out_specs=out_specs, check_vma=False
        )(*args)

    return run
```

```python
import functools

import jax
import jax.numpy as jnp
import numpy as np
from jax import lax
from jax.experimental import pallas as pl
from jax.experimental.pallas import tpu as pltpu
from jax.sharding import PartitionSpec as P

S = 2048
F = 1024
LAGS = 256
BLOCK = 32
CH_DEV = 64
VMEM_GRANT = 60899328


def forward_table():
    freq_index = jnp.arange(F, dtype=jnp.int32)
    time_index = jnp.arange(S, dtype=jnp.int32)
    phase = freq_index[:, None] * time_index[None, :] % S
    angles = phase.astype(jnp.float32) * (2.0 * jnp.pi / S)
    scale = 1.0 / jnp.sqrt(jnp.float32(S))
    return jnp.stack(
        [
            (jnp.cos(angles) * scale).astype(jnp.bfloat16),
            (-jnp.sin(angles) * scale).astype(jnp.bfloat16),
        ],
        axis=1,
    )


def lag_table():
    freq_index = jnp.arange(F, dtype=jnp.int32)
    shifts = (jnp.arange(LAGS, dtype=jnp.int32) - LAGS // 2) % S
    phase = freq_index[:, None] * shifts[None, :] % S
    angles = phase.astype(jnp.float32) * (2.0 * jnp.pi / S)
    scale = 1.0 / jnp.sqrt(jnp.float32(F))
    return jnp.stack(
        [
            (jnp.cos(angles) * scale).astype(jnp.bfloat16),
            (-jnp.sin(angles) * scale).astype(jnp.bfloat16),
        ],
        axis=1,
    )


def synthesize(incoming, table):
    count = incoming.shape[-1]
    flat = incoming.reshape(2 * F, count)
    result = jnp.einsum(
        "qn,qt->tn", flat, table.reshape(2 * F, S), preferred_element_type=jnp.float32
    )
    return result.astype(jnp.bfloat16)


def on_device(records, pairs, observed, lag_mask):
    fibre_count = lax.axis_size("fibre")
    seg_count = lax.axis_size("seg")
    spread_count = fibre_count * seg_count
    freq_dev = F // spread_count
    blocks_dev = CH_DEV // BLOCK
    block_count = CH_DEV * spread_count // BLOCK
    pair_total = pairs.shape[0]
    pairs_dev = pair_total // spread_count
    table = forward_table()
    lags = lag_table()
    spans = records.reshape(1, S // fibre_count, fibre_count, CH_DEV)
    incoming = lax.all_to_all(spans, "fibre", split_axis=2, concat_axis=1, tiled=True)
    count = incoming.shape[3]
    signal = incoming.reshape(S, count)
    result = jnp.einsum(
        "qs,sn->qn", table.reshape(2 * F, S), signal, preferred_element_type=jnp.float32
    )
    spectra = result.reshape(F, 2, count).astype(jnp.bfloat16)
    widened = lax.all_to_all(spectra, ("fibre", "seg"), split_axis=0, concat_axis=2, tiled=True)
    seg_blocks = fibre_count * blocks_dev
    slot_ids = (
        pairs % seg_blocks // blocks_dev * seg_count + pairs // seg_blocks
    ) * blocks_dev + pairs % blocks_dev
    blocks_grid = widened.reshape(freq_dev, 2, block_count, BLOCK)
    first_side = jnp.take(blocks_grid, slot_ids[:, 0], axis=2).astype(jnp.float32)
    second_side = jnp.take(blocks_grid, slot_ids[:, 1], axis=2).astype(jnp.float32)
    first_re, first_im = (first_side[:, 0], first_side[:, 1])
    second_re, second_im = (second_side[:, 0], second_side[:, 1])
    cross_re = first_re * second_re + first_im * second_im
    cross_im = first_im * second_re - first_re * second_im
    cross_spec = jnp.stack([cross_re, cross_im], axis=1).astype(jnp.bfloat16)
    cross_spec = cross_spec.reshape(freq_dev, 2, spread_count, pairs_dev * BLOCK)
    owned_spec = lax.all_to_all(
        cross_spec, ("fibre", "seg"), split_axis=2, concat_axis=0, tiled=True
    )
    owned_spec = owned_spec.reshape(F, 2, pairs_dev * BLOCK)
    partial_corr = jnp.einsum("wpx,wpl->xl", owned_spec, lags, preferred_element_type=jnp.float32)
    synthetic = (
        lax.psum(partial_corr.astype(jnp.bfloat16), "rec")
        .astype(jnp.float32)
        .reshape(pairs_dev, BLOCK, LAGS)
    )
    weights = lag_mask[:, None, :].astype(jnp.float32) * jnp.tanh(synthetic - observed)
    weights_low = weights.astype(jnp.bfloat16).reshape(pairs_dev * BLOCK, LAGS)
    adjoint_spec = jnp.einsum("xl,wpl->wpx", weights_low, lags, preferred_element_type=jnp.float32)
    adjoint_spec = adjoint_spec.astype(jnp.bfloat16).reshape(F, 2, 1, pairs_dev * BLOCK)
    returned = lax.all_to_all(
        adjoint_spec, ("fibre", "seg"), split_axis=0, concat_axis=2, tiled=True
    )
    returned = returned.reshape(freq_dev, 2, pair_total, BLOCK).astype(jnp.float32)
    adjoint_re, adjoint_im = (returned[:, 0], returned[:, 1])
    grad_first = jnp.stack(
        [
            adjoint_re * second_re - adjoint_im * second_im,
            adjoint_re * second_im + adjoint_im * second_re,
        ],
        axis=1,
    )
    grad_second = jnp.stack(
        [
            adjoint_re * first_re + adjoint_im * first_im,
            adjoint_re * first_im - adjoint_im * first_re,
        ],
        axis=1,
    )
    contributions = jnp.concatenate([grad_first, grad_second], axis=2)
    endpoint_ids = jnp.concatenate([slot_ids[:, 0], slot_ids[:, 1]])
    summed = jax.ops.segment_sum(
        jnp.moveaxis(contributions, 2, 0), endpoint_ids, num_segments=block_count
    )
    block_adjoint = jnp.moveaxis(summed, 0, 2).astype(jnp.bfloat16)
    outgoing = block_adjoint.reshape(freq_dev, 2, spread_count, CH_DEV)
    sources = synthesize(
        lax.all_to_all(outgoing, ("fibre", "seg"), split_axis=2, concat_axis=0, tiled=True), table
    )
    regrouped = lax.all_to_all(sources, "fibre", split_axis=0, concat_axis=1, tiled=True)
    return regrouped[None]


def angle_parts(freqs, times, scale):
    phase = (freqs[:, None].astype(np.int64) * times[None, :]) % S
    angles = phase.astype(np.float32) * np.float32(2.0 * np.pi / S)
    return np.stack([np.cos(angles) * scale, -np.sin(angles) * scale])


def band_tables(spread_count):
    order = np.concatenate([np.arange(0, F, 2), np.arange(1, F, 2)]).reshape(spread_count, -1)
    half = np.arange(S // 2)
    scale = np.float32(1.0) / np.sqrt(np.float32(S))
    forward = np.concatenate(
        [angle_parts(band, half, scale).reshape(-1, S // 2) for band in order]
    )
    backward = np.stack([forward[:F].T, forward[F:].T])
    shifts = (np.arange(LAGS) - LAGS // 2) % S
    lag_scale = np.float32(1.0) / np.sqrt(np.float32(F))
    lags = np.stack([angle_parts(band, shifts, lag_scale).reshape(-1, LAGS) for band in order])
    return [table.astype(jnp.bfloat16) for table in (forward, backward, lags)]


def dot(left, right, left_dim=1, right_dim=0):
    return lax.dot_general(
        left,
        right,
        (((left_dim,), (right_dim,)), ((), ())),
        preferred_element_type=jnp.float32,
    )


def fused_kernel(
    sizes, x_hbm, pairs, observed_hbm, mask_hbm, forward_hbm, backward_hbm, lags_hbm, out,
    x, observed, mask, forward, backward, lags, stage1, inbox1, signal, stage2, inbox2, picked, select, cross,
    stage_core, inbox_core, stage3, inbox3, inbox4, stage5, inbox5, stage6, inbox6, load_sem,
    core_sem, relay_send, relay_recv,
    send1, recv1, send2, recv2, send3, recv3, send4, recv4, send5, recv5, send6, recv6,
):
    fibres, segs, recs = sizes
    bands = fibres * segs
    g, f, s, r = (lax.axis_index(name) for name in ("groups", "fibre", "seg", "rec"))
    band = f * segs + s
    span, width = x.shape
    rows = span // 2
    chans = width // fibres
    freqs = F // bands
    low = jnp.bfloat16

    def at(fibre, seg, rec):
        return (g, fibre, seg, rec)

    def at_band(index):
        return at(index // segs, index % segs, r)

    def push(src, dst, send, recv, device):
        copy = pltpu.make_async_remote_copy(
            src_ref=src, dst_ref=dst, send_sem=send, recv_sem=recv,
            device_id=device, device_id_type=pl.DeviceIdType.MESH,
        )
        copy.start()
        return copy

    def arrived(dst, recv):
        pltpu.make_async_remote_copy(
            src_ref=dst, dst_ref=dst, send_sem=recv, recv_sem=recv,
            device_id=at(f, s, 1 - r), device_id_type=pl.DeviceIdType.MESH,
        ).wait_recv()

    def flipped(index, bits):
        result, bit = 0, 1
        while bit < bands:
            digit = index // bit % 2
            result += bit * (1 - digit if bits // bit % 2 else digit)
            bit *= 2
        return result

    partner = at(f, s, 1 - r)
    barrier = pltpu.get_barrier_semaphore()
    for d in range(1, bands):
        pl.semaphore_signal(
            barrier, inc=1, device_id=at_band(flipped(band, d)), device_id_type=pl.DeviceIdType.MESH
        )
    pl.semaphore_signal(barrier, inc=1, device_id=partner, device_id_type=pl.DeviceIdType.MESH)
    sends = []
    first_load = pltpu.make_async_copy(x_hbm, x, load_sem.at[0])
    first_load.start()
    loads = [
        pltpu.make_async_copy(forward_hbm, forward, load_sem.at[1]),
        pltpu.make_async_copy(lags_hbm.at[band], lags, load_sem.at[2]),
        pltpu.make_async_copy(observed_hbm.at[r], observed, load_sem.at[3]),
        pltpu.make_async_copy(mask_hbm, mask, load_sem.at[4]),
        pltpu.make_async_copy(backward_hbm, backward, load_sem.at[5]),
    ]
    first_load.wait()
    for load in loads:
        load.start()
    for j in range(fibres):
        part = x[:, j * chans : (j + 1) * chans]
        stage1[j] = jnp.concatenate([part[:rows], part[rows:]], axis=1)
    pl.semaphore_wait(barrier, bands)
    for d in range(fibres - 1, 0, -1):
        j = flipped(f, d)
        sends.append(push(stage1.at[j], inbox1.at[f], send1.at[d - 1], recv1.at[f], at(j, s, r)))
    inbox1[f] = stage1[f]

    total = select.shape[0]
    count = pairs.shape[1] * BLOCK
    lane = lax.broadcasted_iota(jnp.int32, (1, 2 * count), 1)
    target = lane
    for side in range(2):
        for n in range(pairs.shape[1]):
            first = side * count + n * BLOCK
            n = n % bands * recs + n // bands
            inside = (lane >= first) & (lane < first + BLOCK)
            target = jnp.where(inside, lane + (pairs[side, n] * BLOCK - first), target)
    row = lax.broadcasted_iota(jnp.int32, (total, 2 * count), 0)
    select[...] = jnp.where(row == target, 1.0, 0.0).astype(low)

    for d in range(1, fibres):
        k = (f + d) % fibres
        arrived(inbox1.at[k], recv1.at[k])
    for h in range(fibres // 2):
        early = inbox1[h].astype(jnp.float32)
        late = inbox1[h + fibres // 2].astype(jnp.float32)
        for parity, value in enumerate((early + late, early - late)):
            value = value.astype(low)
            base = parity * (S // 2) + h * span
            signal[base : base + rows] = value[:, :chans]
            signal[base + rows : base + span] = value[:, chans:]

    loads[0].wait()
    half = bands // 2
    for far in (1, 0):
        parity = flipped(f, far * (fibres // 2)) // (fibres // 2)
        top = pl.multiple_of(parity * F, F)
        held = signal[pl.ds(pl.multiple_of(parity * (S // 2), S // 2), S // 2), :]
        for pair in (1, 0):
            inner = flipped(f % 2, pair)
            start = pl.multiple_of(top + inner * (F // 2), F // 2)
            result = dot(forward[pl.ds(start, F // 2), :], held).astype(low)
            for i in range(segs):
                block = result[i * 2 * freqs : (i + 1) * 2 * freqs]
                stage2[parity * half + inner * segs + i] = jnp.concatenate(
                    [block[:freqs], block[freqs:]], axis=1
                )
            first = far * half + pair * segs
            for d in range(first + segs - 1, max(first - 1, 0), -1):
                j = flipped(band, d)
                sends.append(
                    push(stage2.at[j], inbox2.at[band], send2.at[d - 1], recv2.at[band], at_band(j))
                )
    inbox2[band] = stage2[band]
    for d in range(1, bands):
        k = (band + d) % bands
        arrived(inbox2.at[k], recv2.at[k])
    order = [fibre * segs + seg for seg in range(segs) for fibre in range(fibres)]
    spectra = jnp.concatenate(
        [
            jnp.concatenate([inbox2[k][:, p * chans : (p + 1) * chans] for k in order], axis=1)
            for p in range(2)
        ],
        axis=0,
    )
    picked[...] = dot(spectra, select[...])
    share = count // recs
    for h in range(recs):
        a0, a1, b0, b1 = (
            picked[p * freqs : (p + 1) * freqs, side * count + h * share : side * count + (h + 1) * share]
            for side in range(2)
            for p in range(2)
        )
        cross[h] = jnp.concatenate([a0 * b0 + a1 * b1, a1 * b0 - a0 * b1], axis=0).astype(low)
    loads[1].wait()
    stage_core[...] = dot(cross[1 - r], lags[...], 0, 0).astype(low)
    sends.append(push(stage_core, inbox_core, core_sem.at[0], core_sem.at[1], partner))
    partial = dot(cross[r], lags[...], 0, 0)
    arrived(inbox_core, core_sem.at[1])
    partial = (partial + inbox_core[...].astype(jnp.float32)).astype(low)
    stage3[...] = partial.reshape(stage3.shape)
    for d in range(bands - 1, 0, -1):
        j = flipped(band, d)
        sends.append(push(stage3.at[j], inbox3.at[band], send3.at[d - 1], recv3.at[band], at_band(j)))
    inbox3[band] = stage3[band]
    loads[2].wait()
    loads[3].wait()
    for d in range(1, bands):
        k = flipped(band, d)
        arrived(inbox3.at[k], recv3.at[k])
    synthetic = inbox3[0].astype(jnp.float32)
    for k in range(1, bands):
        synthetic += inbox3[k].astype(jnp.float32)
    window = mask[pl.ds(r, 1), :].astype(jnp.float32)
    inbox4[r, band] = (window * jnp.tanh(synthetic - observed[...])).astype(low)
    own = inbox4.at[r, band]
    for d in range(bands - 1, 0, -1):
        j = flipped(band, d)
        sends.append(push(own, own, send4.at[d - 1], recv4.at[band], at_band(j)))
    sends.append(push(own, own, relay_send.at[0], relay_recv.at[band], partner))
    for d in range(1, bands):
        k = flipped(band, d)
        arrived(inbox4.at[r, k], recv4.at[k])
        got = inbox4.at[r, k]
        sends.append(push(got, got, relay_send.at[d], relay_recv.at[k], partner))
    for d in range(bands):
        k = flipped(band, d)
        arrived(inbox4.at[1 - r, k], relay_recv.at[k])
    weights = inbox4[...].reshape(count, LAGS)
    adjoint = dot(lags[...], weights, 1, 1).astype(low).astype(jnp.float32)
    g0, g1 = (adjoint[:freqs], adjoint[freqs:])
    a0, a1 = (picked[:freqs, :count], picked[freqs:, :count])
    b0, b1 = (picked[:freqs, count:], picked[freqs:, count:])
    grads = jnp.concatenate(
        [
            jnp.concatenate([g0 * b0 - g1 * b1, g0 * a0 + g1 * a1], axis=1),
            jnp.concatenate([g0 * b1 + g1 * b0, g0 * a1 - g1 * a0], axis=1),
        ],
        axis=0,
    ).astype(low)
    for far in (1, 0):
        side = flipped(f, far * (fibres // 2)) // (fibres // 2)
        for seg in range(segs):
            start = pl.multiple_of(seg * width + side * (width // 2), width // 2)
            summed = dot(grads, select[pl.ds(start, width // 2), :], 1, 1).astype(low)
            for i in range(fibres // 2):
                cut = slice(i * chans, (i + 1) * chans)
                stage5[(side * (fibres // 2) + i) * segs + seg] = jnp.concatenate(
                    [summed[:freqs, cut], summed[freqs:, cut]], axis=1
                )
        for d in range((far + 1) * half - 1, max(far * half - 1, 0), -1):
            j = flipped(band, d)
            sends.append(
                push(stage5.at[j], inbox5.at[band], send5.at[d - 1], recv5.at[band], at_band(j))
            )
    inbox5[band] = stage5[band]
    loads[4].wait()
    for d in range(1, bands):
        k = (band + d) % bands
        arrived(inbox5.at[k], recv5.at[k])
    held = []
    for parity in range(2):
        pieces = []
        for k in range(parity * bands // 2, (parity + 1) * bands // 2):
            pieces += [inbox5[k][:, :chans], inbox5[k][:, chans:]]
        held.append(jnp.concatenate(pieces, axis=0))
    for i in range(1, -1, -1):
        h = flipped(f, i) % 2
        cut = pl.ds(pl.multiple_of(h * span, span), span)
        even = dot(backward[0, cut, :], held[0])
        odd = dot(backward[1, cut, :], held[1])
        for late, value in enumerate((even + odd, even - odd)):
            value = value.astype(low)
            stage6[h + late * 2] = jnp.concatenate([value[:rows], value[rows:]], axis=1)
        for d in (2 + i, i):
            if d > 0:
                j = flipped(f, d)
                sends.append(push(stage6.at[j], inbox6.at[f], send6.at[d - 1], recv6.at[f], at(j, s, r)))
    inbox6[f] = stage6[f]
    for d in range(1, fibres):
        k = (f + d) % fibres
        arrived(inbox6.at[k], recv6.at[k])
    out[:rows, :] = jnp.concatenate([inbox6[k][:, :chans] for k in range(fibres)], axis=1)
    out[rows:, :] = jnp.concatenate([inbox6[k][:, chans:] for k in range(fibres)], axis=1)
    for copy in sends:
        copy.wait_send()


def fused_on_device(mesh_shape, tables, records, pairs, observed, lag_mask):
    fibres, segs, recs = (mesh_shape[name] for name in ("fibre", "seg", "rec"))
    bands = fibres * segs
    _, span, width = records.shape
    freqs = F // bands
    chans = width // fibres
    count = pairs.shape[0] * BLOCK
    low = jnp.bfloat16
    vmem = pl.BlockSpec(memory_space=pltpu.VMEM)
    hbm = pl.BlockSpec(memory_space=pltpu.HBM)
    row = (freqs, 2 * chans)
    slab = (span // 2, 2 * chans)
    corr = (BLOCK, LAGS)

    def sems(size):
        return [pltpu.SemaphoreType.DMA((size - 1,)), pltpu.SemaphoreType.DMA((size,))]

    result = pl.pallas_call(
        functools.partial(fused_kernel, (fibres, segs, recs)),
        out_shape=pltpu.VMEM((span, width), low),
        in_specs=[hbm, pl.BlockSpec(memory_space=pltpu.SMEM)] + [hbm] * 5,
        out_specs=vmem,
        scratch_shapes=[
            pltpu.VMEM((span, width), low),
            pltpu.VMEM(corr, jnp.float32),
            pltpu.VMEM(lag_mask.shape, jnp.int32),
            pltpu.VMEM((2 * F, S // 2), low),
            pltpu.VMEM((2, S // 2, F), low),
            pltpu.VMEM((2 * freqs, LAGS), low),
            pltpu.VMEM((fibres,) + slab, low),
            pltpu.VMEM((fibres,) + slab, low),
            pltpu.VMEM((S, chans), low),
            pltpu.VMEM((bands,) + row, low),
            pltpu.VMEM((bands,) + row, low),
            pltpu.VMEM((2 * freqs, 2 * count), jnp.float32),
            pltpu.VMEM((segs * width, 2 * count), low),
            pltpu.VMEM((recs, 2 * freqs, count // recs), low),
            pltpu.VMEM((count // recs, LAGS), low),
            pltpu.VMEM((count // recs, LAGS), low),
            pltpu.VMEM((bands,) + corr, low),
            pltpu.VMEM((bands,) + corr, low),
            pltpu.VMEM((recs, bands) + corr, low),
            pltpu.VMEM((bands,) + row, low),
            pltpu.VMEM((bands,) + row, low),
            pltpu.VMEM((fibres,) + slab, low),
            pltpu.VMEM((fibres,) + slab, low),
            pltpu.SemaphoreType.DMA((6,)),
            pltpu.SemaphoreType.DMA((2,)),
            pltpu.SemaphoreType.DMA((bands,)),
            pltpu.SemaphoreType.DMA((bands,)),
            *sems(fibres), *sems(bands), *sems(bands), *sems(bands), *sems(bands), *sems(fibres),
        ],
        compiler_params=pltpu.CompilerParams(
            has_side_effects=True, collective_id=0, vmem_limit_bytes=VMEM_GRANT
        ),
        name="adjoint",
    )(records[0], pairs.T, observed, lag_mask, *tables)
    return result[None]


def fits_fused(shape, records, pairs):
    fibres, segs, recs = (shape[name] for name in ("fibre", "seg", "rec"))
    chans = records.shape[2] // (shape["groups"] * segs * fibres)
    return (
        fibres == 4
        and recs == 2
        and segs & (segs - 1) == 0
        and 2 * chans == 128
        and pairs.shape[0] == fibres * segs * recs
        and F // (fibres * segs) >= 16
    )


def solution(mesh):
    in_specs = (
        P("rec", "fibre", ("groups", "seg")),
        P(),
        P(("groups", "fibre", "seg"), None, None),
        P(("groups", "fibre", "seg"), None),
    )
    out_specs = P("rec", "fibre", ("groups", "seg"))
    shape = dict(mesh.shape)

    def run(records, pairs, observed, lag_mask):
        args = (records, pairs, observed, lag_mask)
        if not fits_fused(shape, records, pairs):
            return jax.shard_map(
                on_device, mesh=mesh, in_specs=in_specs, out_specs=out_specs, check_vma=False
            )(*args)
        tables = [jnp.asarray(t) for t in band_tables(shape["fibre"] * shape["seg"])]

        def body(*blocks):
            return fused_on_device(shape, tables, *blocks)

        return jax.shard_map(
            body, mesh=mesh, in_specs=in_specs, out_specs=out_specs, check_vma=False
        )(*args)

    return run
```
